512 devices in a mesh: cells: 64 (over x, z), feat: 8 (over y, core).
Axes of the slice: x: 4, y: 4, z: 16, core: 2. Of those that a mesh axis runs over, the one named last changes fastest.
Arguments:
- features: float32 [131072, 4096], P('cells', 'feat'), may hold values from -16 to 16
- labels: int32 [131072], P('cells'), may hold values from 0 to 7
- weights: float32 [8, 4096], P(None, 'feat'), may hold values from -0.09375 to 0.09375
Outputs:
- new_weights: float32 [8, 4096], P(None, 'feat')
- new_logits: float32 [8, 131072], P(None, 'cells')
The draws below stay inside these ranges and needn't reach their ends.
All inputs are finite; a program needn't handle non-finite values.
Results may differ from the reference program's by a relative error of at most 0.00018.
Values sent between devices are 32-bit elements; how exact they have to be, the bound alone decides.
No kernel may reach another device: no remote copies, remote signals or barrier semaphores. Data moves between devices by JAX's collectives and lax.ppermute only.
A program may use at most 64 MiB of HBM per device.

```python
import jax
import jax.numpy as jnp
from jax import lax

K = 8
F = 4096
ITERS = 2
NTOT = 131072


def touch_ends(result, rng, low, largest):
    spot = [jax.random.randint(jax.random.fold_in(rng, axis), (), 0, length) for axis, length in enumerate(result.shape)]
    longest = result.shape.index(max(result.shape))
    beside = spot[:longest] + [(spot[longest] + 1) % result.shape[longest]] + spot[longest + 1:]
    return result.at[tuple(spot)].set(low).at[tuple(beside)].set(largest)


def spiked(drawn, own_key, source, target, shards_of, factor):
    owner, partner = [(jnp.arange(drawn.shape[dim]) // (drawn.shape[dim] // shards_of)).reshape([-1 if axis == dim else 1 for axis in range(drawn.ndim)]) for dim in (source, target)]
    chosen = jax.random.permutation(own_key, shards_of)[partner]
    strong = (owner == chosen) | (owner == (partner + shards_of // 2) % shards_of)
    return jnp.where(strong, factor * drawn, drawn)


def levels(own_key, dims, shards, least, top_value):
    loudness = 1.0
    for dim, blocks in shards:
        steps = jax.random.uniform(jax.random.fold_in(jax.random.fold_in(own_key, 6), dim), (blocks,), jnp.float32, least / len(shards), top_value / len(shards))
        loudness = loudness * jnp.repeat(jnp.exp(steps), dims[dim] // blocks).reshape((-1,) + (1,) * (len(dims) - 1 - dim))
    return loudness


def noise(key, dims, deviation, most, split=(), kind=jnp.bfloat16):
    factor_of = levels(key, dims, split, -0.22, 0.18) if split else 1.0
    result = jax.random.normal(key, dims, jnp.float32) * deviation * factor_of
    return jnp.minimum(jnp.maximum(result, -most), most).astype(kind)


def noise_with(stream_key, dims, width, most, split, heavy, kind=jnp.bfloat16):
    entries = width * jax.random.normal(stream_key, dims, jnp.float32)
    if split:
        entries = entries * levels(stream_key, dims, split, -0.22, 0.18)
    return jnp.clip(spiked(entries, jax.random.fold_in(stream_key, 3), *heavy), -most, most).astype(kind)


def setup_inputs(seed: int = 0) -> dict:
    key_list = jax.random.split(jax.random.key(seed), 4)
    features = noise_with(key_list[0], (NTOT, F), 1.0, 16.0, ((0, 64), (1, 8)), (0, 1, 64, 4.0), jnp.float32)
    labels = touch_ends(jax.random.randint(key_list[1], (NTOT,), 0, K), jax.random.fold_in(key_list[1], 1), 0, K - 1).astype(jnp.int32)
    weights = noise(key_list[2], (K, F), F ** -0.5, 0.09375, ((1, 8),), jnp.float32)
    return {"features": features, "labels": labels, "weights": weights}


HIGH = lax.Precision.HIGHEST
RIDGE = 0.01


def scores(coeffs, features):
    return lax.dot_general(coeffs, features, (((1,), (1,)), ((), ())), precision=HIGH, preferred_element_type=jnp.float32)


def reference(features, labels, weights):
    count = features.shape[0] * 1.0
    logits = scores(weights, features)
    expo = jnp.exp(logits)
    probs = expo / jnp.sum(expo, axis=0, keepdims=True)
    onehot = (labels[None, :] == jnp.arange(K, dtype=jnp.int32)[:, None]).astype(jnp.float32)
    grad = jnp.dot(probs - onehot, features, precision=HIGH) / count + RIDGE * weights
    resid = -grad
    direction = resid
    rr_now = jnp.sum(resid * resid)
    step = jnp.zeros_like(weights)
    moved = jnp.zeros_like(logits)
    for it in range(ITERS):
        image = scores(direction, features)
        curv = probs * image - probs * jnp.sum(probs * image, axis=0, keepdims=True)
        product = jnp.dot(curv, features, precision=HIGH) / count + RIDGE * direction
        alpha = rr_now / jnp.sum(direction * product)
        step = step + alpha * direction
        moved = moved + alpha * image
        resid = resid - alpha * product
        if it + 1 < ITERS:
            rr_next = jnp.sum(resid * resid)
            direction = resid + (rr_next / rr_now) * direction
            rr_now = rr_next
    return weights + step, logits + moved
```

```python
import jax
import jax.numpy as jnp
from jax import lax
from jax.sharding import Mesh, PartitionSpec as P

HIGH = lax.Precision.HIGH
RIDGE = 0.01
CELLS = ("x", "z")
FEAT = ("y", "core")


def from_everyone(array, axes):
    devices = lax.axis_size(axes)
    return lax.all_to_all(
        jnp.broadcast_to(array[None], (devices, *array.shape)), axes, 0, 0, tiled=True
    )


def on_device(features, labels, weights):
    rows = features.shape[0]
    classes, width = weights.shape
    count = rows * lax.axis_size(CELLS) * 1.0
    planes = lax.axis_size("x")

    def row_sums(coeffs):
        return lax.dot_general(
            coeffs, features, (((1,), (1,)), ((), ())), precision=HIGH, preferred_element_type=jnp.float32
        )

    def over_feat(local_rows):
        return from_everyone(local_rows, FEAT).sum(axis=0)

    def over_cells(terms):
        local = jnp.dot(terms, features, precision=HIGH, preferred_element_type=jnp.float32)
        blocks = local.reshape(classes, planes, width // planes).transpose(1, 0, 2)
        block = lax.all_to_all(blocks, "x", 0, 0, tiled=True).sum(axis=0)
        block = from_everyone(block, "z").sum(axis=0)
        blocks = from_everyone(block, "x")
        return blocks.transpose(1, 0, 2).reshape(classes, width)

    def with_sums(local_rows, first, second):
        column = lax.broadcasted_iota(jnp.int32, (classes, 128), 1)
        tail = jnp.where(column == 0, first, jnp.where(column == 1, second, jnp.float32(0.0)))
        summed = over_feat(jnp.concatenate([local_rows, tail], axis=1))
        return summed[:, :rows], summed[0, rows], summed[0, rows + 1]

    logits = over_feat(row_sums(weights))
    expo = jnp.exp(logits)
    probs = expo / jnp.sum(expo, axis=0, keepdims=True)
    onehot = (labels[None, :] == jnp.arange(classes, dtype=jnp.int32)[:, None]).astype(jnp.float32)
    resid = -(over_cells(probs - onehot) / count + RIDGE * weights)

    def curved(image):
        return probs * image - probs * jnp.sum(probs * image, axis=0, keepdims=True)

    image, rr0, unused = with_sums(row_sums(resid), jnp.sum(resid * resid), jnp.float32(0.0))
    product = over_cells(curved(image)) / count + RIDGE * resid
    product_image, along, square = with_sums(
        row_sums(product), jnp.sum(resid * product), jnp.sum(product * product)
    )
    alpha0 = rr0 / along
    rr1 = rr0 - 2.0 * alpha0 * along + alpha0 * alpha0 * square
    beta = rr1 / rr0
    direction = resid - alpha0 * product + beta * resid
    direction_image = image - alpha0 * product_image + beta * image
    curvature = jnp.sum(direction_image * curved(direction_image))
    curvature = from_everyone(jnp.full((1, 128), curvature), CELLS)[:, :, :1].sum()
    alpha1 = rr1 / (curvature / count + RIDGE * (rr1 + beta * beta * rr0))
    return (
        weights + (alpha0 * resid + alpha1 * direction),
        logits + (alpha0 * image + alpha1 * direction_image),
    )


def solution(mesh):
    grid = Mesh(mesh.devices.reshape(4, 16, 4, 2), CELLS + FEAT)
    return jax.shard_map(
        on_device,
        mesh=grid,
        in_specs=(P(CELLS, FEAT), P(CELLS), P(None, FEAT)),
        out_specs=(P(None, FEAT), P(None, CELLS)),
        check_vma=False,
    )
```

```python
import functools

import jax
import jax.numpy as jnp
from jax import lax
from jax.experimental import pallas as pl
from jax.experimental.pallas import tpu as pltpu
from jax.sharding import Mesh, PartitionSpec as P

RIDGE = 0.01
CELLS = ("x", "z")
FEAT = ("y", "core")
LANES = 128
CHUNK = 256
F32 = jnp.float32
BF16 = jnp.bfloat16
NN = (((1,), (0,)), ((), ()))
NT = (((1,), (1,)), ((), ()))


def both_parts(value):
    high = value.astype(BF16).astype(F32)
    return jnp.concatenate([high, value - high], axis=0).astype(BF16)


def product_of(parts, high, low, dims):
    k = parts.shape[0] // 2
    one = lax.dot_general(parts, high, dims, preferred_element_type=F32)
    two = lax.dot_general(parts, low, dims, preferred_element_type=F32)
    total = one + two
    return total[:k] + total[k:]


def sum_first(ref, lo=None, hi=None):
    total = ref[0] if lo is None else ref[0, :, lo:hi]
    for i in range(1, ref.shape[0]):
        total = total + (ref[i] if lo is None else ref[i, :, lo:hi])
    return total


def curved(probs, image):
    weighted = probs * image
    return weighted - probs * jnp.sum(weighted, axis=0, keepdims=True)


def total_of(value):
    return jnp.sum(jnp.sum(value, axis=1, keepdims=True), axis=0, keepdims=True)


def tile_of(first, second):
    column = lax.broadcasted_iota(jnp.int32, (8, LANES), 1)
    return jnp.where(column == 0, first, jnp.where(column == 1, second, 0.0))


def spread(ref, value, cols=slice(None)):
    for i in range(ref.shape[0]):
        ref[i, :, cols] = value


def relay_kernel(recv_ref, out_ref):
    spread(out_ref, sum_first(recv_ref))


def first_kernel(w_ref, x_ref, high_ref, low_ref, out_ref, held_w, held, sems):
    steps = held.shape[0] // CHUNK
    copies = []
    weights = pltpu.make_async_copy(w_ref, held_w, sems.at[steps])
    weights.start()
    for i in range(steps):
        rows = pl.ds(i * CHUNK, CHUNK)
        copy = pltpu.make_async_copy(x_ref.at[rows], held.at[rows], sems.at[i])
        copy.start()
        copies.append(copy)
    weights.wait()
    parts = both_parts(held_w[...])
    for i in range(steps):
        rows = pl.ds(i * CHUNK, CHUNK)
        copies[i].wait()
        x = held[rows, :]
        high = x.astype(BF16)
        low = (x - high.astype(F32)).astype(BF16)
        high_ref[rows, :] = high
        low_ref[rows, :] = low
        out_ref[:, rows] = product_of(parts, high, low, NT)


def grad_kernel(recv_ref, labels_ref, high_ref, low_ref, logits_ref, probs_ref, out_ref):
    logits = sum_first(recv_ref)
    logits_ref[...] = logits
    expo = jnp.exp(logits)
    probs = expo / jnp.sum(expo, axis=0, keepdims=True)
    probs_ref[...] = probs
    onehot = (labels_ref[...] == lax.broadcasted_iota(jnp.int32, logits.shape, 0)).astype(F32)
    spread(out_ref, product_of(both_parts(probs - onehot), high_ref[...], low_ref[...], NN))


def resid_kernel(count, recv_ref, w_ref, high_ref, low_ref, resid_ref, out_ref):
    rows = high_ref.shape[0]
    resid = -(sum_first(recv_ref) / count + RIDGE * w_ref[...])
    resid_ref[...] = resid
    out_ref[:, rows:] = tile_of(total_of(resid * resid), 0.0)
    out_ref[:, :rows] = product_of(both_parts(resid), high_ref[...], low_ref[...], NT)


def product_kernel(count, recv_ref, resid_ref, high_ref, low_ref, product_ref, out_ref):
    rows = high_ref.shape[0]
    resid = resid_ref[...]
    product = sum_first(recv_ref) / count + RIDGE * resid
    product_ref[...] = product
    out_ref[:, rows:] = tile_of(total_of(resid * product), total_of(product * product))
    out_ref[:, :rows] = product_of(both_parts(product), high_ref[...], low_ref[...], NT)


def image_kernel(recv_ref, probs_ref, high_ref, low_ref, image_ref, tail_ref, out_ref):
    rows = high_ref.shape[0]
    image = sum_first(recv_ref, 0, rows)
    image_ref[...] = image
    tail_ref[...] = sum_first(recv_ref, rows, rows + LANES)
    terms = curved(probs_ref[...], image)
    spread(out_ref, product_of(both_parts(terms), high_ref[...], low_ref[...], NN))


def scalars(rr0, tail):
    along, square = tail[:1, :1], tail[:1, 1:2]
    alpha = rr0 / along
    rr1 = rr0 - 2.0 * alpha * along + alpha * alpha * square
    return alpha, rr1, rr1 / rr0


def second_kernel(recv_ref, tail_ref, probs_ref, image_ref, direction_ref, tail2_ref, out_ref):
    rows = image_ref.shape[1]
    tail = sum_first(recv_ref, rows, rows + LANES)
    tail2_ref[...] = tail
    alpha, rr1, beta = scalars(tail_ref[:1, :1], tail)
    image = image_ref[...]
    direction = image - alpha * sum_first(recv_ref, 0, rows) + beta * image
    direction_ref[...] = direction
    curvature = total_of(direction * curved(probs_ref[...], direction))
    out_ref[...] = jnp.broadcast_to(curvature, out_ref.shape)


def last_kernel(
    count, curvature_ref, tail_ref, tail2_ref, w_ref, resid_ref, product_ref, logits_ref,
    image_ref, direction_ref, weights_ref, scores_ref,
):
    rr0 = tail_ref[:1, :1]
    alpha, rr1, beta = scalars(rr0, tail2_ref[...])
    curvature = sum_first(curvature_ref)[:, :1]
    alpha1 = rr1 / (curvature / count + RIDGE * (rr1 + beta * beta * rr0))
    resid = resid_ref[...]
    direction = resid - alpha * product_ref[...] + beta * resid
    weights_ref[...] = w_ref[...] + (alpha * resid + alpha1 * direction)
    scores_ref[...] = logits_ref[...] + (alpha * image_ref[...] + alpha1 * direction_ref[...])


def call(kernel, shapes, *args, in_specs=None, scratch=(), limit=4):
    shapes = [jax.ShapeDtypeStruct(s, F32) if isinstance(s, tuple) else s for s in shapes]
    vmem = pl.BlockSpec(memory_space=pltpu.VMEM)
    return pl.pallas_call(
        kernel,
        out_shape=shapes,
        in_specs=in_specs or [vmem] * len(args),
        out_specs=[vmem] * len(shapes),
        scratch_shapes=list(scratch),
        compiler_params=pltpu.CompilerParams(vmem_limit_bytes=limit * 1024 * 1024),
    )(*args)


def exchange(blocks, axes):
    return lax.all_to_all(blocks, axes, 0, 0, tiled=True)


def relay(recv, axis):
    (blocks,) = call(relay_kernel, [(lax.axis_size(axis), *recv.shape[1:])], recv)
    return exchange(blocks, axis)


def over_feat(partial):
    return relay(lax.all_gather(partial, "core"), "y")


def over_cells(blocks):
    return relay(exchange(blocks, "z"), "x")


def on_device(features, labels, weights):
    rows, width = features.shape
    classes = weights.shape[0]
    count = rows * lax.axis_size(CELLS) * 1.0
    split = pltpu.VMEM((rows, width), BF16)
    cells, coeffs = (classes, rows), (classes, width)
    blocks = (lax.axis_size("z"), classes, width)
    padded, tile = (classes, rows + LANES), (classes, LANES)

    high, low, partial = call(
        first_kernel,
        [split, split, pltpu.VMEM(cells, F32)],
        weights,
        features,
        in_specs=[pl.BlockSpec(memory_space=pltpu.HBM)] * 2,
        limit=50,
        scratch=[
            pltpu.VMEM(coeffs, F32),
            pltpu.VMEM((rows, width), F32),
            pltpu.SemaphoreType.DMA((rows // CHUNK + 1,)),
        ],
    )
    logits, probs, partial = call(
        grad_kernel, [cells, cells, blocks], over_feat(partial), labels.reshape(1, rows), high, low
    )
    resid, partial = call(
        functools.partial(resid_kernel, count), [coeffs, padded], over_cells(partial), weights, high, low
    )
    image, tail, partial = call(
        image_kernel, [cells, tile, blocks], over_feat(partial), probs, high, low
    )
    product, partial = call(
        functools.partial(product_kernel, count), [coeffs, padded], over_cells(partial), resid, high, low
    )
    direction, tail2, curvature = call(
        second_kernel, [cells, tile, (lax.axis_size(CELLS), 1, LANES)], over_feat(partial), tail, probs, image
    )
    curvature = exchange(curvature, CELLS)
    return tuple(
        call(
            functools.partial(last_kernel, count),
            [coeffs, cells],
            curvature, tail, tail2, weights, resid, product, logits, image, direction,
        )
    )


def solution(mesh):
    grid = Mesh(mesh.devices.reshape(4, 16, 4, 2), CELLS + FEAT)
    return jax.shard_map(
        on_device,
        mesh=grid,
        in_specs=(P(CELLS, FEAT), P(CELLS), P(None, FEAT)),
        out_specs=(P(None, FEAT), P(None, CELLS)),
        check_vma=False,
    )
```

```python
import functools

import jax
import jax.numpy as jnp
from jax import lax
from jax.experimental import pallas as pl
from jax.experimental.pallas import tpu as pltpu
from jax.sharding import Mesh, PartitionSpec as P

RIDGE = 0.01
CELLS = ("x", "z")
FEAT = ("y", "core")
LANES = 128
CHUNK = 256
F32 = jnp.float32
BF16 = jnp.bfloat16
NN = (((1,), (0,)), ((), ()))
NT = (((1,), (1,)), ((), ()))


def both_parts(value):
    high = value.astype(BF16).astype(F32)
    return jnp.concatenate([high, value - high], axis=0).astype(BF16)


def product_of(parts, high, low, dims):
    k = parts.shape[0] // 2
    one = lax.dot_general(parts, high, dims, preferred_element_type=F32)
    two = lax.dot_general(parts, low, dims, preferred_element_type=F32)
    total = one + two
    return total[:k] + total[k:]


def sum_first(ref, lo=None, hi=None):
    total = ref[0] if lo is None else ref[0, :, lo:hi]
    for i in range(1, ref.shape[0]):
        total = total + (ref[i] if lo is None else ref[i, :, lo:hi])
    return total


def joined(ref):
    return jnp.concatenate([ref[i] for i in range(ref.shape[0])], axis=1)


def curved(probs, image):
    weighted = probs * image
    return weighted - probs * jnp.sum(weighted, axis=0, keepdims=True)


def total_of(value):
    return jnp.sum(jnp.sum(value, axis=1, keepdims=True), axis=0, keepdims=True)


def tile_of(first, second):
    column = lax.broadcasted_iota(jnp.int32, (8, LANES), 1)
    return jnp.where(column == 0, first, jnp.where(column == 1, second, 0.0))


def spread(ref, value):
    for i in range(ref.shape[0]):
        ref[i] = value


def spread_blocks(ref, value):
    step = value.shape[1] // ref.shape[0]
    for i in range(ref.shape[0]):
        ref[i] = value[:, i * step : (i + 1) * step]


def relay_kernel(recv_ref, out_ref):
    spread(out_ref, sum_first(recv_ref))


def first_kernel(w_ref, x_ref, high_ref, low_ref, out_ref, held_w, held, sems):
    steps = held.shape[0] // CHUNK
    copies = []
    weights = pltpu.make_async_copy(w_ref, held_w, sems.at[steps])
    weights.start()
    for i in range(steps):
        rows = pl.ds(i * CHUNK, CHUNK)
        copy = pltpu.make_async_copy(x_ref.at[rows], held.at[rows], sems.at[i])
        copy.start()
        copies.append(copy)
    weights.wait()
    parts = both_parts(held_w[...])
    for i in range(steps):
        rows = pl.ds(i * CHUNK, CHUNK)
        copies[i].wait()
        x = held[rows, :]
        high = x.astype(BF16)
        low = (x - high.astype(F32)).astype(BF16)
        high_ref[rows, :] = high
        low_ref[rows, :] = low
        out_ref[:, rows] = product_of(parts, high, low, NT)


def grad_kernel(recv_ref, labels_ref, high_ref, low_ref, logits_ref, probs_ref, out_ref):
    logits = sum_first(recv_ref)
    logits_ref[...] = logits
    expo = jnp.exp(logits)
    probs = expo / jnp.sum(expo, axis=0, keepdims=True)
    probs_ref[...] = probs
    onehot = (labels_ref[...] == lax.broadcasted_iota(jnp.int32, logits.shape, 0)).astype(F32)
    spread_blocks(out_ref, product_of(both_parts(probs - onehot), high_ref[...], low_ref[...], NN))


def resid_kernel(count, recv_ref, w_ref, high_ref, low_ref, resid_ref, out_ref):
    rows = high_ref.shape[0]
    resid = -(joined(recv_ref) / count + RIDGE * w_ref[...])
    resid_ref[...] = resid
    out_ref[:, rows:] = tile_of(total_of(resid * resid), 0.0)
    out_ref[:, :rows] = product_of(both_parts(resid), high_ref[...], low_ref[...], NT)


def product_kernel(count, recv_ref, resid_ref, high_ref, low_ref, product_ref, out_ref):
    rows = high_ref.shape[0]
    resid = resid_ref[...]
    product = joined(recv_ref) / count + RIDGE * resid
    product_ref[...] = product
    out_ref[:, rows:] = tile_of(total_of(resid * product), total_of(product * product))
    out_ref[:, :rows] = product_of(both_parts(product), high_ref[...], low_ref[...], NT)


def image_kernel(recv_ref, probs_ref, high_ref, low_ref, image_ref, tail_ref, out_ref):
    rows = high_ref.shape[0]
    image = sum_first(recv_ref, 0, rows)
    image_ref[...] = image
    tail_ref[...] = sum_first(recv_ref, rows, rows + LANES)
    terms = curved(probs_ref[...], image)
    spread_blocks(out_ref, product_of(both_parts(terms), high_ref[...], low_ref[...], NN))


def scalars(rr0, tail):
    along, square = tail[:1, :1], tail[:1, 1:2]
    alpha = rr0 / along
    rr1 = rr0 - 2.0 * alpha * along + alpha * alpha * square
    return alpha, rr1, rr1 / rr0


def second_kernel(recv_ref, tail_ref, probs_ref, image_ref, direction_ref, tail2_ref, out_ref):
    rows = image_ref.shape[1]
    tail = sum_first(recv_ref, rows, rows + LANES)
    tail2_ref[...] = tail
    alpha, rr1, beta = scalars(tail_ref[:1, :1], tail)
    image = image_ref[...]
    direction = image - alpha * sum_first(recv_ref, 0, rows) + beta * image
    direction_ref[...] = direction
    curvature = total_of(direction * curved(probs_ref[...], direction))
    out_ref[...] = jnp.broadcast_to(curvature, out_ref.shape)


def last_kernel(
    count, curvature_ref, tail_ref, tail2_ref, w_ref, resid_ref, product_ref, logits_ref,
    image_ref, direction_ref, weights_ref, scores_ref,
):
    rr0 = tail_ref[:1, :1]
    alpha, rr1, beta = scalars(rr0, tail2_ref[...])
    curvature = sum_first(curvature_ref)[:, :1]
    alpha1 = rr1 / (curvature / count + RIDGE * (rr1 + beta * beta * rr0))
    resid = resid_ref[...]
    direction = resid - alpha * product_ref[...] + beta * resid
    weights_ref[...] = w_ref[...] + (alpha * resid + alpha1 * direction)
    scores_ref[...] = logits_ref[...] + (alpha * image_ref[...] + alpha1 * direction_ref[...])


def call(kernel, shapes, *args, in_specs=None, scratch=(), limit=4):
    shapes = [jax.ShapeDtypeStruct(s, F32) if isinstance(s, tuple) else s for s in shapes]
    vmem = pl.BlockSpec(memory_space=pltpu.VMEM)
    return pl.pallas_call(
        kernel,
        out_shape=shapes,
        in_specs=in_specs or [vmem] * len(args),
        out_specs=[vmem] * len(shapes),
        scratch_shapes=list(scratch),
        compiler_params=pltpu.CompilerParams(vmem_limit_bytes=limit * 1024 * 1024),
    )(*args)


def exchange(blocks, axes):
    return lax.all_to_all(blocks, axes, 0, 0, tiled=True)


def relay(recv, axis):
    (blocks,) = call(relay_kernel, [(lax.axis_size(axis), *recv.shape[1:])], recv)
    return exchange(blocks, axis)


def over_feat(partial):
    return relay(lax.all_gather(partial, "core"), "y")


def over_cells(blocks):
    return relay(relay(exchange(blocks, "x"), "z"), "x")


def on_device(features, labels, weights):
    rows, width = features.shape
    classes = weights.shape[0]
    count = rows * lax.axis_size(CELLS) * 1.0
    split = pltpu.VMEM((rows, width), BF16)
    cells, coeffs = (classes, rows), (classes, width)
    planes = lax.axis_size("x")
    blocks = (planes, classes, width // planes)
    padded, tile = (classes, rows + LANES), (classes, LANES)

    high, low, partial = call(
        first_kernel,
        [split, split, pltpu.VMEM(cells, F32)],
        weights,
        features,
        in_specs=[pl.BlockSpec(memory_space=pltpu.HBM)] * 2,
        limit=50,
        scratch=[
            pltpu.VMEM(coeffs, F32),
            pltpu.VMEM((rows, width), F32),
            pltpu.SemaphoreType.DMA((rows // CHUNK + 1,)),
        ],
    )
    logits, probs, partial = call(
        grad_kernel, [cells, cells, blocks], over_feat(partial), labels.reshape(1, rows), high, low
    )
    resid, partial = call(
        functools.partial(resid_kernel, count), [coeffs, padded], over_cells(partial), weights, high, low
    )
    image, tail, partial = call(
        image_kernel, [cells, tile, blocks], over_feat(partial), probs, high, low
    )
    product, partial = call(
        functools.partial(product_kernel, count), [coeffs, padded], over_cells(partial), resid, high, low
    )
    direction, tail2, curvature = call(
        second_kernel, [cells, tile, (lax.axis_size(CELLS), 1, LANES)], over_feat(partial), tail, probs, image
    )
    curvature = exchange(curvature, CELLS)
    return tuple(
        call(
            functools.partial(last_kernel, count),
            [coeffs, cells],
            curvature, tail, tail2, weights, resid, product, logits, image, direction,
        )
    )


def solution(mesh):
    grid = Mesh(mesh.devices.reshape(4, 16, 4, 2), CELLS + FEAT)
    return jax.shard_map(
        on_device,
        mesh=grid,
        in_specs=(P(CELLS, FEAT), P(CELLS), P(None, FEAT)),
        out_specs=(P(None, FEAT), P(None, CELLS)),
        check_vma=False,
    )
```

```python
import functools

import jax
import jax.numpy as jnp
import numpy as np
from jax import lax
from jax.experimental import pallas as pl
from jax.experimental.pallas import tpu as pltpu
from jax.sharding import Mesh, PartitionSpec as P

RIDGE = 0.01
CELLS = ("x", "z")
GRID = ("x", "z", "y", "core")
FEAT = ("y", "core")
LANES = 128
CHUNK = 512
F32 = jnp.float32
BF16 = jnp.bfloat16
NN = (((1,), (0,)), ((), ()))
NT = (((1,), (1,)), ((), ()))


def both_parts(value):
    high = value.astype(BF16).astype(F32)
    return jnp.concatenate([high, value - high], axis=0).astype(BF16)


def product_of(parts, high, low, dims):
    k = parts.shape[0] // 2
    one = lax.dot_general(parts, high, dims, preferred_element_type=F32)
    two = lax.dot_general(parts, low, dims, preferred_element_type=F32)
    total = one + two
    return total[:k] + total[k:]


def sum_first(ref, lo=None, hi=None):
    total = ref[0] if lo is None else ref[0, :, lo:hi]
    for i in range(1, ref.shape[0]):
        total = total + (ref[i] if lo is None else ref[i, :, lo:hi])
    return total


def joined(ref):
    return jnp.concatenate([ref[i] for i in range(ref.shape[0])], axis=1)


def curved(probs, image):
    weighted = probs * image
    return weighted - probs * jnp.sum(weighted, axis=0, keepdims=True)


def total_of(value):
    return jnp.sum(jnp.sum(value, axis=1, keepdims=True), axis=0, keepdims=True)


def tile_of(first, second):
    column = lax.broadcasted_iota(jnp.int32, (8, LANES), 1)
    return jnp.where(column == 0, first, jnp.where(column == 1, second, 0.0))


def spread(ref, value):
    for i in range(ref.shape[0]):
        ref[i] = value


def spread_blocks(ref, value):
    step = value.shape[1] // ref.shape[0]
    for i in range(ref.shape[0]):
        ref[i] = value[:, i * step : (i + 1) * step]


def relay_kernel(recv_ref, out_ref):
    spread(out_ref, sum_first(recv_ref))


def chip_rows(value, parts_of):
    (high0, low0), (high1, low1) = parts_of
    half = value.shape[1] // 2
    left = product_of(both_parts(value[:, :half]), high0[...], low0[...], NT)
    return left + product_of(both_parts(value[:, half:]), high1[...], low1[...], NT)


def chip_columns(ref, value, parts_of):
    parts = both_parts(value)
    halves = [product_of(parts, high[...], low[...], NN) for high, low in parts_of]
    spread_blocks(ref, jnp.concatenate(halves, axis=1))


def first_kernel(w_ref, x_ref, high_ref, low_ref, out_ref, held_w, held, sems):
    total = held.shape[0]
    steps = total // CHUNK
    copies = []
    weights = pltpu.make_async_copy(w_ref, held_w, sems.at[steps])
    weights.start()
    for i in range(steps):
        rows = pl.ds(i * CHUNK, CHUNK)
        copy = pltpu.make_async_copy(x_ref.at[rows], held.at[rows], sems.at[i])
        copy.start()
        copies.append(copy)
    weights.wait()
    parts = both_parts(held_w[...])
    out_ref[:, total:] = held_w[...]
    for i in range(steps):
        rows = pl.ds(i * CHUNK, CHUNK)
        copies[i].wait()
        x = held[rows, :]
        high = x.astype(BF16)
        low = (x - high.astype(F32)).astype(BF16)
        high_ref[rows, :] = high
        low_ref[rows, :] = low
        out_ref[:, rows] = product_of(parts, high, low, NT)


def chip_kernel(recv_ref, weights_ref, out_ref):
    rows = out_ref.shape[2]
    weights_ref[...] = jnp.concatenate([recv_ref[0, :, rows:], recv_ref[1, :, rows:]], axis=1)
    spread(out_ref, sum_first(recv_ref, 0, rows))


def grad_kernel(
    recv_ref, labels_ref, moved_ref, high1_ref, low1_ref,
    logits_ref, probs_ref, out_ref, high0_ref, low0_ref,
):
    x = moved_ref[...]
    high = x.astype(BF16)
    high0_ref[...] = high
    low0_ref[...] = (x - high.astype(F32)).astype(BF16)
    logits = sum_first(recv_ref)
    logits_ref[...] = logits
    expo = jnp.exp(logits)
    probs = expo / jnp.sum(expo, axis=0, keepdims=True)
    probs_ref[...] = probs
    onehot = (labels_ref[...] == lax.broadcasted_iota(jnp.int32, logits.shape, 0)).astype(F32)
    chip_columns(out_ref, probs - onehot, ((high0_ref, low0_ref), (high1_ref, low1_ref)))


def send_rows(out_ref, value, tile, parts_of):
    rows = out_ref.shape[2] - LANES
    image = chip_rows(value, parts_of)
    for i in range(out_ref.shape[0]):
        out_ref[i, :, :rows] = image
        out_ref[i, :, rows:] = tile


def resid_kernel(count, recv_ref, w_ref, high0, low0, high1, low1, resid_ref, out_ref):
    resid = -(joined(recv_ref) / count + RIDGE * w_ref[...])
    resid_ref[...] = resid
    tile = tile_of(total_of(resid * resid), 0.0)
    send_rows(out_ref, resid, tile, ((high0, low0), (high1, low1)))


def product_kernel(count, recv_ref, resid_ref, high0, low0, high1, low1, product_ref, out_ref):
    resid = resid_ref[...]
    product = joined(recv_ref) / count + RIDGE * resid
    product_ref[...] = product
    tile = tile_of(total_of(resid * product), total_of(product * product))
    send_rows(out_ref, product, tile, ((high0, low0), (high1, low1)))


def image_kernel(recv_ref, probs_ref, high0, low0, high1, low1, image_ref, tail_ref, out_ref):
    rows = image_ref.shape[1]
    image = sum_first(recv_ref, 0, rows)
    image_ref[...] = image
    tail_ref[...] = sum_first(recv_ref, rows, rows + LANES)
    chip_columns(out_ref, curved(probs_ref[...], image), ((high0, low0), (high1, low1)))


def scalars(rr0, tail):
    along, square = tail[:1, :1], tail[:1, 1:2]
    alpha = rr0 / along
    rr1 = rr0 - 2.0 * alpha * along + alpha * alpha * square
    return alpha, rr1, rr1 / rr0


def second_kernel(recv_ref, tail_ref, probs_ref, image_ref, direction_ref, tail2_ref, out_ref):
    rows = image_ref.shape[1]
    tail = sum_first(recv_ref, rows, rows + LANES)
    tail2_ref[...] = tail
    alpha, rr1, beta = scalars(tail_ref[:1, :1], tail)
    image = image_ref[...]
    direction = image - alpha * sum_first(recv_ref, 0, rows) + beta * image
    direction_ref[...] = direction
    curvature = total_of(direction * curved(probs_ref[...], direction))
    out_ref[...] = jnp.broadcast_to(curvature, out_ref.shape)


def last_kernel(
    count, curvature_ref, tail_ref, tail2_ref, w_ref, resid_ref, product_ref, logits_ref,
    image_ref, direction_ref, out_ref,
):
    rows = logits_ref.shape[1]
    rr0 = tail_ref[:1, :1]
    alpha, rr1, beta = scalars(rr0, tail2_ref[...])
    curvature = sum_first(curvature_ref)[:, :1]
    alpha1 = rr1 / (curvature / count + RIDGE * (rr1 + beta * beta * rr0))
    resid = resid_ref[...]
    direction = resid - alpha * product_ref[...] + beta * resid
    out_ref[:, rows:] = w_ref[...] + (alpha * resid + alpha1 * direction)
    out_ref[:, :rows] = logits_ref[...] + (alpha * image_ref[...] + alpha1 * direction_ref[...])


def share_kernel(recv_ref, weights_ref, scores_ref):
    rows, width = scores_ref.shape[1], weights_ref.shape[1]
    scores_ref[...] = recv_ref[1, :, :rows]
    start = pl.multiple_of(rows + width * lax.axis_index("core"), LANES)
    weights_ref[...] = recv_ref[1, :, pl.ds(start, width)]


def call(kernel, shapes, *args, in_specs=None, scratch=(), limit=4):
    shapes = [jax.ShapeDtypeStruct(s, F32) if isinstance(s, tuple) else s for s in shapes]
    vmem = pl.BlockSpec(memory_space=pltpu.VMEM)
    return pl.pallas_call(
        kernel,
        out_shape=shapes,
        in_specs=in_specs or [vmem] * len(args),
        out_specs=[vmem] * len(shapes),
        scratch_shapes=list(scratch),
        compiler_params=pltpu.CompilerParams(vmem_limit_bytes=limit * 1024 * 1024),
    )(*args)


def groups(kind):
    nx, nz, ny, nc = (lax.axis_size(axis) for axis in GRID)
    place = np.arange(nx * nz * ny * nc).reshape(nx, nz, ny, nc)
    near, work = place[..., 0], place[..., 1]
    xyz = near.transpose(1, 0, 2)
    if kind == "x":
        pair = work.transpose(2, 1, 0).reshape(-1, nx), near.reshape(-1, ny)
    elif kind == "y":
        pair = work.reshape(-1, ny), near.transpose(1, 2, 0).reshape(-1, nx)
    elif kind == "z":
        pair = work.transpose(0, 2, 1).reshape(-1, nz), xyz.reshape(-1, nx * ny)
    else:
        pair = work.transpose(2, 0, 1).reshape(ny, -1), xyz.reshape(ny, -1)
    return np.concatenate(pair).tolist()


def exchange(blocks, kind):
    return lax.all_to_all(blocks, GRID, 0, 0, axis_index_groups=groups(kind), tiled=True)


def relay(recv, axis):
    (blocks,) = call(relay_kernel, [(lax.axis_size(axis), *recv.shape[1:])], recv)
    return exchange(blocks, axis)


def over_cells(blocks):
    return relay(relay(exchange(blocks, "x"), "z"), "x")


def on_device(features, labels, weights):
    rows, width = features.shape
    classes = weights.shape[0]
    count = rows * lax.axis_size(CELLS) * 1.0
    split = pltpu.VMEM((rows, width), BF16)
    planes, lines = lax.axis_size("x"), lax.axis_size("y")
    cells, coeffs, tile = (classes, rows), (classes, 2 * width), (classes, LANES)
    blocks = (planes, classes, 2 * width // planes)
    padded = (lines, classes, rows + LANES)

    moved = lax.ppermute(features, "core", [(0, 1)])
    high1, low1, partial = call(
        first_kernel,
        [split, split, pltpu.VMEM((classes, rows + width), F32)],
        weights,
        features,
        in_specs=[pl.BlockSpec(memory_space=pltpu.HBM)] * 2,
        limit=51,
        scratch=[
            pltpu.VMEM((classes, width), F32),
            pltpu.VMEM((rows, width), F32),
            pltpu.SemaphoreType.DMA((rows // CHUNK + 1,)),
        ],
    )
    weights, partial = call(
        chip_kernel, [coeffs, (lines, *cells)], lax.all_gather(partial, "core")
    )
    logits, probs, partial, high0, low0 = call(
        grad_kernel,
        [cells, cells, blocks, split, split],
        exchange(partial, "y"), labels.reshape(1, rows), moved, high1, low1,
    )
    parts = (high0, low0, high1, low1)
    resid, partial = call(
        functools.partial(resid_kernel, count), [coeffs, padded], over_cells(partial), weights, *parts
    )
    image, tail, partial = call(
        image_kernel, [cells, tile, blocks], exchange(partial, "y"), probs, *parts
    )
    product, partial = call(
        functools.partial(product_kernel, count), [coeffs, padded], over_cells(partial), resid, *parts
    )
    direction, tail2, curvature = call(
        second_kernel,
        [cells, tile, (lax.axis_size(CELLS), 1, LANES)],
        exchange(partial, "y"), tail, probs, image,
    )
    (result,) = call(
        functools.partial(last_kernel, count),
        [(classes, rows + 2 * width)],
        exchange(curvature, "cells"), tail, tail2, weights, resid, product, logits, image, direction,
    )
    return tuple(
        call(share_kernel, [(classes, width), cells], lax.all_gather(result, "core"))
    )


def solution(mesh):
    grid = Mesh(mesh.devices.reshape(4, 16, 4, 2), GRID)
    return jax.shard_map(
        on_device,
        mesh=grid,
        in_specs=(P(CELLS, FEAT), P(CELLS), P(None, FEAT)),
        out_specs=(P(None, FEAT), P(None, CELLS)),
        check_vma=False,
    )
```

```python
import functools

import jax
import jax.numpy as jnp
import numpy as np
from jax import lax
from jax.experimental import pallas as pl
from jax.experimental.pallas import tpu as pltpu
from jax.sharding import Mesh, PartitionSpec as P

RIDGE = 0.01
CELLS = ("x", "z")
GRID = ("x", "z", "y", "core")
FEAT = ("y", "core")
LANES = 128
CHUNK = 512
F32 = jnp.float32
BF16 = jnp.bfloat16
NN = (((1,), (0,)), ((), ()))
NT = (((1,), (1,)), ((), ()))


def both_parts(value):
    high = value.astype(BF16).astype(F32)
    return jnp.concatenate([high, value - high], axis=0).astype(BF16)


def product_of(parts, high, low, dims):
    k = parts.shape[0] // 2
    one = lax.dot_general(parts, high, dims, preferred_element_type=F32)
    two = lax.dot_general(parts, low, dims, preferred_element_type=F32)
    total = one + two
    return total[:k] + total[k:]


def sum_first(ref, lo=None, hi=None):
    total = ref[0] if lo is None else ref[0, :, lo:hi]
    for i in range(1, ref.shape[0]):
        total = total + (ref[i] if lo is None else ref[i, :, lo:hi])
    return total


def joined(ref):
    return jnp.concatenate([ref[i] for i in range(ref.shape[0])], axis=1)


def curved(probs, image):
    weighted = probs * image
    return weighted - probs * jnp.sum(weighted, axis=0, keepdims=True)


def total_of(value):
    return jnp.sum(jnp.sum(value, axis=1, keepdims=True), axis=0, keepdims=True)


def tile_of(first, second):
    column = lax.broadcasted_iota(jnp.int32, (8, LANES), 1)
    return jnp.where(column == 0, first, jnp.where(column == 1, second, 0.0))


def spread(ref, value):
    for i in range(ref.shape[0]):
        ref[i] = value


def spread_blocks(ref, value):
    step = value.shape[1] // ref.shape[0]
    for i in range(ref.shape[0]):
        ref[i] = value[:, i * step : (i + 1) * step]


def relay_kernel(recv_ref, out_ref):
    spread(out_ref, sum_first(recv_ref))


def chip_rows(value, parts_of):
    (high0, low0), (high1, low1) = parts_of
    half = value.shape[1] // 2
    left = product_of(both_parts(value[:, :half]), high0[...], low0[...], NT)
    return left + product_of(both_parts(value[:, half:]), high1[...], low1[...], NT)


def chip_columns(ref, value, parts_of):
    parts = both_parts(value)
    halves = [product_of(parts, high[...], low[...], NN) for high, low in parts_of]
    spread_blocks(ref, jnp.concatenate(halves, axis=1))


def first_kernel(w_ref, x_ref, high_ref, low_ref, out_ref, held, held_w, sems):
    total = held.shape[0]
    steps = total // CHUNK
    copies = []
    weights = pltpu.make_async_copy(w_ref, held_w, sems.at[steps])
    weights.start()
    for i in range(steps):
        rows = pl.ds(i * CHUNK, CHUNK)
        copy = pltpu.make_async_copy(x_ref.at[rows], held.at[rows], sems.at[i])
        copy.start()
        copies.append(copy)
    weights.wait()
    parts = both_parts(held_w[...])
    out_ref[:, total:] = held_w[...]
    for i in range(steps):
        rows = pl.ds(i * CHUNK, CHUNK)
        copies[i].wait()
        x = held[rows, :]
        high = x.astype(BF16)
        low = (x - high.astype(F32)).astype(BF16)
        high_ref[rows, :] = high
        low_ref[rows, :] = low
        out_ref[:, rows] = product_of(parts, high, low, NT)


def chip_kernel(recv_ref, weights_ref, out_ref):
    rows = out_ref.shape[2]
    weights_ref[...] = jnp.concatenate([recv_ref[0, :, rows:], recv_ref[1, :, rows:]], axis=1)
    spread(out_ref, sum_first(recv_ref, 0, rows))


def grad_kernel(
    recv_ref, labels_ref, moved_ref, high1_ref, low1_ref,
    logits_ref, probs_ref, out_ref, high0_ref, low0_ref,
):
    x = moved_ref[...]
    high = x.astype(BF16)
    high0_ref[...] = high
    low0_ref[...] = (x - high.astype(F32)).astype(BF16)
    logits = sum_first(recv_ref)
    logits_ref[...] = logits
    expo = jnp.exp(logits)
    probs = expo / jnp.sum(expo, axis=0, keepdims=True)
    probs_ref[...] = probs
    onehot = (labels_ref[...] == lax.broadcasted_iota(jnp.int32, logits.shape, 0)).astype(F32)
    chip_columns(out_ref, probs - onehot, ((high0_ref, low0_ref), (high1_ref, low1_ref)))


def send_rows(out_ref, value, tile, parts_of):
    rows = out_ref.shape[2] - LANES
    image = chip_rows(value, parts_of)
    for i in range(out_ref.shape[0]):
        out_ref[i, :, :rows] = image
        out_ref[i, :, rows:] = tile


def resid_kernel(count, recv_ref, w_ref, high0, low0, high1, low1, resid_ref, out_ref):
    resid = -(joined(recv_ref) / count + RIDGE * w_ref[...])
    resid_ref[...] = resid
    tile = tile_of(total_of(resid * resid), 0.0)
    send_rows(out_ref, resid, tile, ((high0, low0), (high1, low1)))


def product_kernel(count, recv_ref, resid_ref, high0, low0, high1, low1, product_ref, out_ref):
    resid = resid_ref[...]
    product = joined(recv_ref) / count + RIDGE * resid
    product_ref[...] = product
    tile = tile_of(total_of(resid * product), total_of(product * product))
    send_rows(out_ref, product, tile, ((high0, low0), (high1, low1)))


def image_kernel(recv_ref, probs_ref, high0, low0, high1, low1, image_ref, tail_ref, out_ref):
    rows = image_ref.shape[1]
    image = sum_first(recv_ref, 0, rows)
    image_ref[...] = image
    tail_ref[...] = sum_first(recv_ref, rows, rows + LANES)
    chip_columns(out_ref, curved(probs_ref[...], image), ((high0, low0), (high1, low1)))


def scalars(rr0, tail):
    along, square = tail[:1, :1], tail[:1, 1:2]
    alpha = rr0 / along
    rr1 = rr0 - 2.0 * alpha * along + alpha * alpha * square
    return alpha, rr1, rr1 / rr0


def second_kernel(recv_ref, tail_ref, probs_ref, image_ref, direction_ref, tail2_ref, out_ref):
    rows = image_ref.shape[1]
    tail = sum_first(recv_ref, rows, rows + LANES)
    tail2_ref[...] = tail
    alpha, rr1, beta = scalars(tail_ref[:1, :1], tail)
    image = image_ref[...]
    direction = image - alpha * sum_first(recv_ref, 0, rows) + beta * image
    direction_ref[...] = direction
    curvature = total_of(direction * curved(probs_ref[...], direction))
    out_ref[...] = jnp.broadcast_to(curvature, out_ref.shape)


def last_kernel(
    count, curvature_ref, tail_ref, tail2_ref, w_ref, resid_ref, product_ref, logits_ref,
    image_ref, direction_ref, out_ref,
):
    rows = logits_ref.shape[1]
    rr0 = tail_ref[:1, :1]
    alpha, rr1, beta = scalars(rr0, tail2_ref[...])
    curvature = sum_first(curvature_ref)[:, :1]
    alpha1 = rr1 / (curvature / count + RIDGE * (rr1 + beta * beta * rr0))
    resid = resid_ref[...]
    direction = resid - alpha * product_ref[...] + beta * resid
    out_ref[:, rows:] = w_ref[...] + (alpha * resid + alpha1 * direction)
    out_ref[:, :rows] = logits_ref[...] + (alpha * image_ref[...] + alpha1 * direction_ref[...])


def share_kernel(recv_ref, weights_ref, scores_ref):
    rows, width = scores_ref.shape[1], weights_ref.shape[1]
    scores_ref[...] = recv_ref[1, :, :rows]
    start = pl.multiple_of(rows + width * lax.axis_index("core"), LANES)
    weights_ref[...] = recv_ref[1, :, pl.ds(start, width)]


def call(kernel, shapes, *args, in_specs=None, scratch=(), limit=4):
    shapes = [jax.ShapeDtypeStruct(s, F32) if isinstance(s, tuple) else s for s in shapes]
    vmem = pl.BlockSpec(memory_space=pltpu.VMEM)
    return pl.pallas_call(
        kernel,
        out_shape=shapes,
        in_specs=in_specs or [vmem] * len(args),
        out_specs=[vmem] * len(shapes),
        scratch_shapes=list(scratch),
        compiler_params=pltpu.CompilerParams(vmem_limit_bytes=limit * 1024 * 1024),
    )(*args)


def groups(kind):
    nx, nz, ny, nc = (lax.axis_size(axis) for axis in GRID)
    place = np.arange(nx * nz * ny * nc).reshape(nx, nz, ny, nc)
    near, work = place[..., 0], place[..., 1]
    xyz = near.transpose(1, 0, 2)
    if kind == "x":
        pair = work.transpose(2, 1, 0).reshape(-1, nx), near.reshape(-1, ny)
    elif kind == "y":
        pair = work.reshape(-1, ny), near.transpose(1, 2, 0).reshape(-1, nx)
    elif kind == "z":
        pair = work.transpose(0, 2, 1).reshape(-1, nz), xyz.reshape(-1, nx * ny)
    else:
        pair = work.transpose(2, 0, 1).reshape(ny, -1), xyz.reshape(ny, -1)
    return np.concatenate(pair).tolist()


def exchange(blocks, kind):
    return lax.all_to_all(blocks, GRID, 0, 0, axis_index_groups=groups(kind), tiled=True)


def relay(recv, axis):
    (blocks,) = call(relay_kernel, [(lax.axis_size(axis), *recv.shape[1:])], recv)
    return exchange(blocks, axis)


def over_cells(blocks):
    return relay(relay(exchange(blocks, "x"), "z"), "x")


def on_device(features, labels, weights):
    rows, width = features.shape
    classes = weights.shape[0]
    count = rows * lax.axis_size(CELLS) * 1.0
    split = pltpu.VMEM((rows, width), BF16)
    planes, lines = lax.axis_size("x"), lax.axis_size("y")
    cells, coeffs, tile = (classes, rows), (classes, 2 * width), (classes, LANES)
    blocks = (planes, classes, 2 * width // planes)
    padded = (lines, classes, rows + LANES)

    high1, low1, partial, held = call(
        first_kernel,
        [
            split,
            split,
            pltpu.VMEM((classes, rows + width), F32),
            pltpu.VMEM((rows, width), F32),
        ],
        weights,
        features,
        in_specs=[pl.BlockSpec(memory_space=pltpu.HBM)] * 2,
        limit=49,
        scratch=[
            pltpu.VMEM((classes, width), F32),
            pltpu.SemaphoreType.DMA((rows // CHUNK + 1,)),
        ],
    )
    gathered, held = lax.optimization_barrier((lax.all_gather(partial, "core"), held))
    moved = lax.ppermute(held, "core", [(0, 1)])
    weights, partial = call(chip_kernel, [coeffs, (lines, *cells)], gathered)
    logits, probs, partial, high0, low0 = call(
        grad_kernel,
        [cells, cells, blocks, split, split],
        exchange(partial, "y"), labels.reshape(1, rows), moved, high1, low1,
    )
    parts = (high0, low0, high1, low1)
    resid, partial = call(
        functools.partial(resid_kernel, count), [coeffs, padded], over_cells(partial), weights, *parts
    )
    image, tail, partial = call(
        image_kernel, [cells, tile, blocks], exchange(partial, "y"), probs, *parts
    )
    product, partial = call(
        functools.partial(product_kernel, count), [coeffs, padded], over_cells(partial), resid, *parts
    )
    direction, tail2, curvature = call(
        second_kernel,
        [cells, tile, (lax.axis_size(CELLS), 1, LANES)],
        exchange(partial, "y"), tail, probs, image,
    )
    (result,) = call(
        functools.partial(last_kernel, count),
        [(classes, rows + 2 * width)],
        exchange(curvature, "cells"), tail, tail2, weights, resid, product, logits, image, direction,
    )
    return tuple(
        call(share_kernel, [(classes, width), cells], lax.all_gather(result, "core"))
    )


def solution(mesh):
    grid = Mesh(mesh.devices.reshape(4, 16, 4, 2), GRID)
    return jax.shard_map(
        on_device,
        mesh=grid,
        in_specs=(P(CELLS, FEAT), P(CELLS), P(None, FEAT)),
        out_specs=(P(None, FEAT), P(None, CELLS)),
        check_vma=False,
    )
```

```python
import functools

import jax
import jax.numpy as jnp
import numpy as np
from jax import lax
from jax.experimental import pallas as pl
from jax.experimental.pallas import tpu as pltpu
from jax.sharding import Mesh, PartitionSpec as P

RIDGE = 0.01
CELLS = ("x", "z")
GRID = ("x", "z", "y", "core")
FEAT = ("y", "core")
LANES = 128
CHUNK = 512
F32 = jnp.float32
BF16 = jnp.bfloat16
NN = (((1,), (0,)), ((), ()))
NT = (((1,), (1,)), ((), ()))


def both_parts(value):
    high = value.astype(BF16).astype(F32)
    return jnp.concatenate([high, value - high], axis=0).astype(BF16)


def product_of(parts, high, low, dims):
    k = parts.shape[0] // 2
    one = lax.dot_general(parts, high, dims, preferred_element_type=F32)
    two = lax.dot_general(parts, low, dims, preferred_element_type=F32)
    total = one + two
    return total[:k] + total[k:]


def sum_first(ref, lo=None, hi=None):
    total = ref[0] if lo is None else ref[0, :, lo:hi]
    for i in range(1, ref.shape[0]):
        total = total + (ref[i] if lo is None else ref[i, :, lo:hi])
    return total


def joined(ref, width):
    pieces = width // ref.shape[2]
    line = ref.shape[0] // pieces
    return jnp.concatenate(
        [sum_first(ref.at[pl.ds(i * line, line)]) for i in range(pieces)], axis=1
    )


def curved(probs, image):
    weighted = probs * image
    return weighted - probs * jnp.sum(weighted, axis=0, keepdims=True)


def total_of(value):
    return jnp.sum(jnp.sum(value, axis=1, keepdims=True), axis=0, keepdims=True)


def tile_of(first, second):
    column = lax.broadcasted_iota(jnp.int32, (8, LANES), 1)
    return jnp.where(column == 0, first, jnp.where(column == 1, second, 0.0))


def spread(ref, value):
    for i in range(ref.shape[0]):
        ref[i] = value


def spread_blocks(ref, value):
    step = value.shape[1] // ref.shape[0]
    for i in range(ref.shape[0]):
        ref[i] = value[:, i * step : (i + 1) * step]


def relay_kernel(recv_ref, out_ref):
    spread(out_ref, sum_first(recv_ref))


def chip_rows(value, parts_of):
    (high0, low0), (high1, low1) = parts_of
    half = value.shape[1] // 2
    left = product_of(both_parts(value[:, :half]), high0[...], low0[...], NT)
    return left + product_of(both_parts(value[:, half:]), high1[...], low1[...], NT)


def chip_columns(ref, value, parts_of):
    parts = both_parts(value)
    halves = [product_of(parts, high[...], low[...], NN) for high, low in parts_of]
    spread_blocks(ref, jnp.concatenate(halves, axis=1))


def first_kernel(w_ref, x_ref, high_ref, low_ref, out_ref, held, held_w, sems):
    total = held.shape[0]
    steps = total // CHUNK
    copies = []
    weights = pltpu.make_async_copy(w_ref, held_w, sems.at[steps])
    weights.start()
    for i in range(steps):
        rows = pl.ds(i * CHUNK, CHUNK)
        copy = pltpu.make_async_copy(x_ref.at[rows], held.at[rows], sems.at[i])
        copy.start()
        copies.append(copy)
    weights.wait()
    parts = both_parts(held_w[...])
    out_ref[:, total:] = held_w[...]
    for i in range(steps):
        rows = pl.ds(i * CHUNK, CHUNK)
        copies[i].wait()
        x = held[rows, :]
        high = x.astype(BF16)
        low = (x - high.astype(F32)).astype(BF16)
        high_ref[rows, :] = high
        low_ref[rows, :] = low
        out_ref[:, rows] = product_of(parts, high, low, NT)


def chip_kernel(recv_ref, weights_ref, out_ref):
    rows = out_ref.shape[2]
    weights_ref[...] = jnp.concatenate([recv_ref[0, :, rows:], recv_ref[1, :, rows:]], axis=1)
    spread(out_ref, sum_first(recv_ref, 0, rows))


def grad_kernel(
    recv_ref, labels_ref, moved_ref, high1_ref, low1_ref,
    logits_ref, probs_ref, out_ref, high0_ref, low0_ref,
):
    x = moved_ref[...]
    high = x.astype(BF16)
    high0_ref[...] = high
    low0_ref[...] = (x - high.astype(F32)).astype(BF16)
    logits = sum_first(recv_ref)
    logits_ref[...] = logits
    expo = jnp.exp(logits)
    probs = expo / jnp.sum(expo, axis=0, keepdims=True)
    probs_ref[...] = probs
    onehot = (labels_ref[...] == lax.broadcasted_iota(jnp.int32, logits.shape, 0)).astype(F32)
    chip_columns(out_ref, probs - onehot, ((high0_ref, low0_ref), (high1_ref, low1_ref)))


def send_rows(out_ref, value, tile, parts_of):
    rows = out_ref.shape[2] - LANES
    image = chip_rows(value, parts_of)
    for i in range(out_ref.shape[0]):
        out_ref[i, :, :rows] = image
        out_ref[i, :, rows:] = tile


def resid_kernel(count, recv_ref, w_ref, high0, low0, high1, low1, resid_ref, out_ref):
    resid = -(joined(recv_ref, w_ref.shape[1]) / count + RIDGE * w_ref[...])
    resid_ref[...] = resid
    tile = tile_of(total_of(resid * resid), 0.0)
    send_rows(out_ref, resid, tile, ((high0, low0), (high1, low1)))


def product_kernel(count, recv_ref, resid_ref, high0, low0, high1, low1, product_ref, out_ref):
    resid = resid_ref[...]
    product = joined(recv_ref, resid.shape[1]) / count + RIDGE * resid
    product_ref[...] = product
    tile = tile_of(total_of(resid * product), total_of(product * product))
    send_rows(out_ref, product, tile, ((high0, low0), (high1, low1)))


def image_kernel(recv_ref, probs_ref, high0, low0, high1, low1, image_ref, tail_ref, out_ref):
    rows = image_ref.shape[1]
    image = sum_first(recv_ref, 0, rows)
    image_ref[...] = image
    tail_ref[...] = sum_first(recv_ref, rows, rows + LANES)
    chip_columns(out_ref, curved(probs_ref[...], image), ((high0, low0), (high1, low1)))


def scalars(rr0, tail):
    along, square = tail[:1, :1], tail[:1, 1:2]
    alpha = rr0 / along
    rr1 = rr0 - 2.0 * alpha * along + alpha * alpha * square
    return alpha, rr1, rr1 / rr0


def second_kernel(recv_ref, tail_ref, probs_ref, image_ref, direction_ref, tail2_ref, out_ref):
    rows = image_ref.shape[1]
    tail = sum_first(recv_ref, rows, rows + LANES)
    tail2_ref[...] = tail
    alpha, rr1, beta = scalars(tail_ref[:1, :1], tail)
    image = image_ref[...]
    direction = image - alpha * sum_first(recv_ref, 0, rows) + beta * image
    direction_ref[...] = direction
    curvature = total_of(direction * curved(probs_ref[...], direction))
    out_ref[...] = jnp.broadcast_to(curvature, out_ref.shape)


def last_kernel(
    count, curvature_ref, tail_ref, tail2_ref, w_ref, resid_ref, product_ref, logits_ref,
    image_ref, direction_ref, out_ref,
):
    rows = logits_ref.shape[1]
    rr0 = tail_ref[:1, :1]
    alpha, rr1, beta = scalars(rr0, tail2_ref[...])
    curvature = sum_first(curvature_ref)[:, :1]
    alpha1 = rr1 / (curvature / count + RIDGE * (rr1 + beta * beta * rr0))
    resid = resid_ref[...]
    direction = resid - alpha * product_ref[...] + beta * resid
    out_ref[:, rows:] = w_ref[...] + (alpha * resid + alpha1 * direction)
    out_ref[:, :rows] = logits_ref[...] + (alpha * image_ref[...] + alpha1 * direction_ref[...])


def share_kernel(recv_ref, weights_ref, scores_ref):
    rows, width = scores_ref.shape[1], weights_ref.shape[1]
    scores_ref[...] = recv_ref[1, :, :rows]
    start = pl.multiple_of(rows + width * lax.axis_index("core"), LANES)
    weights_ref[...] = recv_ref[1, :, pl.ds(start, width)]


def call(kernel, shapes, *args, in_specs=None, scratch=(), limit=4):
    shapes = [jax.ShapeDtypeStruct(s, F32) if isinstance(s, tuple) else s for s in shapes]
    vmem = pl.BlockSpec(memory_space=pltpu.VMEM)
    return pl.pallas_call(
        kernel,
        out_shape=shapes,
        in_specs=in_specs or [vmem] * len(args),
        out_specs=[vmem] * len(shapes),
        scratch_shapes=list(scratch),
        compiler_params=pltpu.CompilerParams(vmem_limit_bytes=limit * 1024 * 1024),
    )(*args)


def groups(kind):
    nx, nz, ny, nc = (lax.axis_size(axis) for axis in GRID)
    place = np.arange(nx * nz * ny * nc).reshape(nx, nz, ny, nc)
    near, work = place[..., 0], place[..., 1]
    xyz = near.transpose(1, 0, 2)
    if kind == "x":
        pair = work.transpose(2, 1, 0).reshape(-1, nx), near.reshape(-1, ny)
    elif kind == "y":
        pair = work.reshape(-1, ny), near.transpose(1, 2, 0).reshape(-1, nx)
    elif kind == "z":
        pair = work.transpose(0, 2, 1).reshape(-1, nz), xyz.reshape(-1, nx * ny)
    else:
        pair = work.transpose(2, 0, 1).reshape(ny, -1), xyz.reshape(ny, -1)
    return np.concatenate(pair).tolist()


def exchange(blocks, kind):
    return lax.all_to_all(blocks, GRID, 0, 0, axis_index_groups=groups(kind), tiled=True)


def over_cells(blocks):
    recv = exchange(blocks, "x")
    (blocks,) = call(relay_kernel, [(lax.axis_size(CELLS), *recv.shape[1:])], recv)
    return exchange(blocks, "cells")


def on_device(features, labels, weights):
    rows, width = features.shape
    classes = weights.shape[0]
    count = rows * lax.axis_size(CELLS) * 1.0
    split = pltpu.VMEM((rows, width), BF16)
    planes, lines = lax.axis_size("x"), lax.axis_size("y")
    cells, coeffs, tile = (classes, rows), (classes, 2 * width), (classes, LANES)
    blocks = (planes, classes, 2 * width // planes)
    padded = (lines, classes, rows + LANES)

    high1, low1, partial, held = call(
        first_kernel,
        [
            split,
            split,
            pltpu.VMEM((classes, rows + width), F32),
            pltpu.VMEM((rows, width), F32),
        ],
        weights,
        features,
        in_specs=[pl.BlockSpec(memory_space=pltpu.HBM)] * 2,
        limit=49,
        scratch=[
            pltpu.VMEM((classes, width), F32),
            pltpu.SemaphoreType.DMA((rows // CHUNK + 1,)),
        ],
    )
    gathered, held = lax.optimization_barrier((lax.all_gather(partial, "core"), held))
    moved = lax.ppermute(held, "core", [(0, 1)])
    weights, partial = call(chip_kernel, [coeffs, (lines, *cells)], gathered)
    logits, probs, partial, high0, low0 = call(
        grad_kernel,
        [cells, cells, blocks, split, split],
        exchange(partial, "y"), labels.reshape(1, rows), moved, high1, low1,
    )
    parts = (high0, low0, high1, low1)
    resid, partial = call(
        functools.partial(resid_kernel, count), [coeffs, padded], over_cells(partial), weights, *parts
    )
    image, tail, partial = call(
        image_kernel, [cells, tile, blocks], exchange(partial, "y"), probs, *parts
    )
    product, partial = call(
        functools.partial(product_kernel, count), [coeffs, padded], over_cells(partial), resid, *parts
    )
    direction, tail2, curvature = call(
        second_kernel,
        [cells, tile, (lax.axis_size(CELLS), 1, LANES)],
        exchange(partial, "y"), tail, probs, image,
    )
    (result,) = call(
        functools.partial(last_kernel, count),
        [(classes, rows + 2 * width)],
        exchange(curvature, "cells"), tail, tail2, weights, resid, product, logits, image, direction,
    )
    return tuple(
        call(share_kernel, [(classes, width), cells], lax.all_gather(result, "core"))
    )


def solution(mesh):
    grid = Mesh(mesh.devices.reshape(4, 16, 4, 2), GRID)
    return jax.shard_map(
        on_device,
        mesh=grid,
        in_specs=(P(CELLS, FEAT), P(CELLS), P(None, FEAT)),
        out_specs=(P(None, FEAT), P(None, CELLS)),
        check_vma=False,
    )
```

```python
import functools

import jax
import jax.numpy as jnp
import numpy as np
from jax import lax
from jax.experimental import pallas as pl
from jax.experimental.pallas import tpu as pltpu
from jax.sharding import Mesh, PartitionSpec as P

RIDGE = 0.01
CELLS = ("x", "z")
GRID = ("x", "z", "y", "core")
FEAT = ("y", "core")
LANES = 128
CHUNK = 512
F32 = jnp.float32
BF16 = jnp.bfloat16
NN = (((1,), (0,)), ((), ()))
NT = (((1,), (1,)), ((), ()))


def both_parts(value):
    high = value.astype(BF16).astype(F32)
    return jnp.concatenate([high, value - high], axis=0).astype(BF16)


def product_of(parts, high, low, dims):
    k = parts.shape[0] // 2
    one = lax.dot_general(parts, high, dims, preferred_element_type=F32)
    two = lax.dot_general(parts, low, dims, preferred_element_type=F32)
    total = one + two
    return total[:k] + total[k:]


def sum_first(ref, lo=None, hi=None):
    total = ref[0] if lo is None else ref[0, :, lo:hi]
    for i in range(1, ref.shape[0]):
        total = total + (ref[i] if lo is None else ref[i, :, lo:hi])
    return total


def joined(ref):
    return jnp.concatenate([ref[i] for i in range(ref.shape[0])], axis=1)


def curved(probs, image):
    weighted = probs * image
    return weighted - probs * jnp.sum(weighted, axis=0, keepdims=True)


def total_of(value):
    return jnp.sum(jnp.sum(value, axis=1, keepdims=True), axis=0, keepdims=True)


def tile_of(first, second):
    column = lax.broadcasted_iota(jnp.int32, (8, LANES), 1)
    return jnp.where(column == 0, first, jnp.where(column == 1, second, 0.0))


def spread(ref, value):
    for i in range(ref.shape[0]):
        ref[i] = value


def spread_blocks(ref, value):
    step = value.shape[1] // ref.shape[0]
    for i in range(ref.shape[0]):
        ref[i] = value[:, i * step : (i + 1) * step]


def relay_kernel(recv_ref, out_ref):
    spread(out_ref, sum_first(recv_ref))


def chip_rows(value, parts_of):
    (high0, low0), (high1, low1) = parts_of
    half = value.shape[1] // 2
    left = product_of(both_parts(value[:, :half]), high0[...], low0[...], NT)
    return left + product_of(both_parts(value[:, half:]), high1[...], low1[...], NT)


def chip_columns(ref, value, parts_of):
    parts = both_parts(value)
    halves = [product_of(parts, high[...], low[...], NN) for high, low in parts_of]
    spread_blocks(ref, jnp.concatenate(halves, axis=1))


def first_kernel(w_ref, x_ref, high_ref, low_ref, out_ref, held, held_w, sems):
    total = held.shape[0]
    steps = total // CHUNK
    copies = []
    weights = pltpu.make_async_copy(w_ref, held_w, sems.at[steps])
    weights.start()
    for i in range(steps):
        rows = pl.ds(i * CHUNK, CHUNK)
        copy = pltpu.make_async_copy(x_ref.at[rows], held.at[rows], sems.at[i])
        copy.start()
        copies.append(copy)
    weights.wait()
    parts = both_parts(held_w[...])
    out_ref[:, total:] = held_w[...]
    for i in range(steps):
        rows = pl.ds(i * CHUNK, CHUNK)
        copies[i].wait()
        x = held[rows, :]
        high = x.astype(BF16)
        low = (x - high.astype(F32)).astype(BF16)
        high_ref[rows, :] = high
        low_ref[rows, :] = low
        out_ref[:, rows] = product_of(parts, high, low, NT)


def chip_kernel(recv_ref, weights_ref, out_ref):
    rows = out_ref.shape[2]
    weights_ref[...] = jnp.concatenate([recv_ref[0, :, rows:], recv_ref[1, :, rows:]], axis=1)
    spread(out_ref, sum_first(recv_ref, 0, rows))


def grad_kernel(recv_ref, labels_ref, high1, low1, logits_ref, probs_ref, parts_ref, half_ref):
    logits = sum_first(recv_ref)
    logits_ref[...] = logits
    expo = jnp.exp(logits)
    probs = expo / jnp.sum(expo, axis=0, keepdims=True)
    probs_ref[...] = probs
    onehot = (labels_ref[...] == lax.broadcasted_iota(jnp.int32, logits.shape, 0)).astype(F32)
    parts = both_parts(probs - onehot)
    parts_ref[...] = parts
    half_ref[...] = product_of(parts, high1[...], low1[...], NN)


def moved_kernel(parts_ref, half_ref, moved_ref, out_ref, high0_ref, low0_ref):
    x = moved_ref[...]
    high = x.astype(BF16)
    high0_ref[...] = high
    low0_ref[...] = (x - high.astype(F32)).astype(BF16)
    first = product_of(parts_ref[...], high0_ref[...], low0_ref[...], NN)
    spread_blocks(out_ref, jnp.concatenate([first, half_ref[...]], axis=1))


def send_rows(out_ref, value, tile, parts_of):
    rows = out_ref.shape[2] - LANES
    image = chip_rows(value, parts_of)
    for i in range(out_ref.shape[0]):
        out_ref[i, :, :rows] = image
        out_ref[i, :, rows:] = tile


def resid_kernel(count, recv_ref, w_ref, high0, low0, high1, low1, resid_ref, out_ref):
    resid = -(joined(recv_ref) / count + RIDGE * w_ref[...])
    resid_ref[...] = resid
    tile = tile_of(total_of(resid * resid), 0.0)
    send_rows(out_ref, resid, tile, ((high0, low0), (high1, low1)))


def product_kernel(count, recv_ref, resid_ref, high0, low0, high1, low1, product_ref, out_ref):
    resid = resid_ref[...]
    product = joined(recv_ref) / count + RIDGE * resid
    product_ref[...] = product
    tile = tile_of(total_of(resid * product), total_of(product * product))
    send_rows(out_ref, product, tile, ((high0, low0), (high1, low1)))


def image_kernel(recv_ref, probs_ref, high0, low0, high1, low1, image_ref, tail_ref, out_ref):
    rows = image_ref.shape[1]
    image = sum_first(recv_ref, 0, rows)
    image_ref[...] = image
    tail_ref[...] = sum_first(recv_ref, rows, rows + LANES)
    chip_columns(out_ref, curved(probs_ref[...], image), ((high0, low0), (high1, low1)))


def scalars(rr0, tail):
    along, square = tail[:1, :1], tail[:1, 1:2]
    alpha = rr0 / along
    rr1 = jnp.maximum(rr0 - 2.0 * alpha * along + alpha * alpha * square, 0.0)
    return alpha, rr1, rr1 / rr0


def second_kernel(recv_ref, tail_ref, probs_ref, image_ref, direction_ref, tail2_ref, out_ref):
    rows = image_ref.shape[1]
    tail = sum_first(recv_ref, rows, rows + LANES)
    tail2_ref[...] = tail
    alpha, rr1, beta = scalars(tail_ref[:1, :1], tail)
    image = image_ref[...]
    direction = image - alpha * sum_first(recv_ref, 0, rows) + beta * image
    direction_ref[...] = direction
    curvature = total_of(direction * curved(probs_ref[...], direction))
    out_ref[...] = jnp.broadcast_to(curvature, out_ref.shape)


def last_kernel(
    count, curvature_ref, tail_ref, tail2_ref, w_ref, resid_ref, product_ref, logits_ref,
    image_ref, direction_ref, out_ref,
):
    rows = logits_ref.shape[1]
    rr0 = tail_ref[:1, :1]
    alpha, rr1, beta = scalars(rr0, tail2_ref[...])
    curvature = sum_first(curvature_ref)[:, :1]
    bent = curvature / count + RIDGE * (rr1 + beta * beta * rr0)
    alpha1 = jnp.where(rr1 > 0.0, rr1 / bent, 0.0)
    resid = resid_ref[...]
    direction = resid - alpha * product_ref[...] + beta * resid
    out_ref[:, rows:] = w_ref[...] + (alpha * resid + alpha1 * direction)
    out_ref[:, :rows] = logits_ref[...] + (alpha * image_ref[...] + alpha1 * direction_ref[...])


def share_kernel(recv_ref, weights_ref, scores_ref):
    rows, width = scores_ref.shape[1], weights_ref.shape[1]
    scores_ref[...] = recv_ref[1, :, :rows]
    start = pl.multiple_of(rows + width * lax.axis_index("core"), LANES)
    weights_ref[...] = recv_ref[1, :, pl.ds(start, width)]


def call(kernel, shapes, *args, in_specs=None, scratch=(), limit=4):
    shapes = [jax.ShapeDtypeStruct(s, F32) if isinstance(s, tuple) else s for s in shapes]
    vmem = pl.BlockSpec(memory_space=pltpu.VMEM)
    return pl.pallas_call(
        kernel,
        out_shape=shapes,
        in_specs=in_specs or [vmem] * len(args),
        out_specs=[vmem] * len(shapes),
        scratch_shapes=list(scratch),
        compiler_params=pltpu.CompilerParams(vmem_limit_bytes=limit * 1024 * 1024),
    )(*args)


def groups(kind):
    nx, nz, ny, nc = (lax.axis_size(axis) for axis in GRID)
    place = np.arange(nx * nz * ny * nc).reshape(nx, nz, ny, nc)
    near, work = place[..., 0], place[..., 1]
    xyz = near.transpose(1, 0, 2)
    if kind == "x":
        pair = work.transpose(2, 1, 0).reshape(-1, nx), near.reshape(-1, ny)
    elif kind == "y":
        pair = work.reshape(-1, ny), near.transpose(1, 2, 0).reshape(-1, nx)
    elif kind == "z":
        pair = work.transpose(0, 2, 1).reshape(-1, nz), xyz.reshape(-1, nx * ny)
    else:
        pair = work.transpose(2, 0, 1).reshape(ny, -1), xyz.reshape(ny, -1)
    return np.concatenate(pair).tolist()


def exchange(blocks, kind):
    return lax.all_to_all(blocks, GRID, 0, 0, axis_index_groups=groups(kind), tiled=True)


def relay(recv, axis):
    (blocks,) = call(relay_kernel, [(lax.axis_size(axis), *recv.shape[1:])], recv)
    return exchange(blocks, axis)


def over_cells(blocks):
    return relay(relay(exchange(blocks, "x"), "z"), "x")


def on_device(features, labels, weights):
    rows, width = features.shape
    classes = weights.shape[0]
    count = rows * lax.axis_size(CELLS) * 1.0
    split = pltpu.VMEM((rows, width), BF16)
    planes, lines = lax.axis_size("x"), lax.axis_size("y")
    cells, coeffs, tile = (classes, rows), (classes, 2 * width), (classes, LANES)
    blocks = (planes, classes, 2 * width // planes)
    padded = (lines, classes, rows + LANES)

    high1, low1, partial, held = call(
        first_kernel,
        [
            split,
            split,
            pltpu.VMEM((classes, rows + width), F32),
            pltpu.VMEM((rows, width), F32),
        ],
        weights,
        features,
        in_specs=[pl.BlockSpec(memory_space=pltpu.HBM)] * 2,
        limit=49,
        scratch=[
            pltpu.VMEM((classes, width), F32),
            pltpu.SemaphoreType.DMA((rows // CHUNK + 1,)),
        ],
    )
    gathered, held = lax.optimization_barrier((lax.all_gather(partial, "core"), held))
    moved = lax.ppermute(held, "core", [(0, 1)])
    weights, partial = call(chip_kernel, [coeffs, (lines, *cells)], gathered)
    logits, probs, terms, half = call(
        grad_kernel,
        [cells, cells, pltpu.VMEM((2 * classes, rows), BF16), (classes, width)],
        exchange(partial, "y"), labels.reshape(1, rows), high1, low1,
    )
    partial, high0, low0 = call(moved_kernel, [blocks, split, split], terms, half, moved)
    parts = (high0, low0, high1, low1)
    resid, partial = call(
        functools.partial(resid_kernel, count), [coeffs, padded], over_cells(partial), weights, *parts
    )
    image, tail, partial = call(
        image_kernel, [cells, tile, blocks], exchange(partial, "y"), probs, *parts
    )
    product, partial = call(
        functools.partial(product_kernel, count), [coeffs, padded], over_cells(partial), resid, *parts
    )
    direction, tail2, curvature = call(
        second_kernel,
        [cells, tile, (lax.axis_size(CELLS), 1, LANES)],
        exchange(partial, "y"), tail, probs, image,
    )
    (result,) = call(
        functools.partial(last_kernel, count),
        [(classes, rows + 2 * width)],
        exchange(curvature, "cells"), tail, tail2, weights, resid, product, logits, image, direction,
    )
    return tuple(
        call(share_kernel, [(classes, width), cells], lax.all_gather(result, "core"))
    )


def solution(mesh):
    grid = Mesh(mesh.devices.reshape(4, 16, 4, 2), GRID)
    return jax.shard_map(
        on_device,
        mesh=grid,
        in_specs=(P(CELLS, FEAT), P(CELLS), P(None, FEAT)),
        out_specs=(P(None, FEAT), P(None, CELLS)),
        check_vma=False,
    )
```

```python
import functools

import jax
import jax.numpy as jnp
import numpy as np
from jax import lax
from jax.experimental import pallas as pl
from jax.experimental.pallas import tpu as pltpu
from jax.sharding import Mesh, PartitionSpec as P

RIDGE = 0.01
CELLS = ("x", "z")
GRID = ("x", "z", "y", "core")
FEAT = ("y", "core")
LANES = 128
CHUNK = 512
F32 = jnp.float32
BF16 = jnp.bfloat16
NN = (((1,), (0,)), ((), ()))
NT = (((1,), (1,)), ((), ()))


def both_parts(value):
    high = value.astype(BF16).astype(F32)
    return jnp.concatenate([high, value - high], axis=0).astype(BF16)


def product_of(parts, high, low, dims):
    k = parts.shape[0] // 2
    one = lax.dot_general(parts, high, dims, preferred_element_type=F32)
    two = lax.dot_general(parts, low, dims, preferred_element_type=F32)
    total = one + two
    return total[:k] + total[k:]


def sum_first(ref, lo=None, hi=None):
    total = ref[0] if lo is None else ref[0, :, lo:hi]
    for i in range(1, ref.shape[0]):
        total = total + (ref[i] if lo is None else ref[i, :, lo:hi])
    return total


def joined(ref):
    return jnp.concatenate([ref[i] for i in range(ref.shape[0])], axis=1)


def curved(probs, image):
    weighted = probs * image
    return weighted - probs * jnp.sum(weighted, axis=0, keepdims=True)


def total_of(value):
    return jnp.sum(jnp.sum(value, axis=1, keepdims=True), axis=0, keepdims=True)


def tile_of(*values):
    column = lax.broadcasted_iota(jnp.int32, (8, LANES), 1)
    tile = jnp.zeros((8, LANES), F32)
    for i, value in enumerate(values):
        tile = jnp.where(column == i, value, tile)
    return tile


def spread(ref, value):
    for i in range(ref.shape[0]):
        ref[i] = value


def spread_blocks(ref, value):
    step = value.shape[1] // ref.shape[0]
    for i in range(ref.shape[0]):
        ref[i] = value[:, i * step : (i + 1) * step]


def relay_kernel(recv_ref, out_ref):
    spread(out_ref, sum_first(recv_ref))


def chip_rows(value, parts_of):
    (high0, low0), (high1, low1) = parts_of
    half = value.shape[1] // 2
    left = product_of(both_parts(value[:, :half]), high0[...], low0[...], NT)
    return left + product_of(both_parts(value[:, half:]), high1[...], low1[...], NT)


def chip_columns(ref, value, parts_of):
    parts = both_parts(value)
    halves = [product_of(parts, high[...], low[...], NN) for high, low in parts_of]
    spread_blocks(ref, jnp.concatenate(halves, axis=1))


def first_kernel(w_ref, x_ref, high_ref, low_ref, out_ref, held, held_w, sems):
    total = held.shape[0]
    steps = total // CHUNK
    copies = []
    weights = pltpu.make_async_copy(w_ref, held_w, sems.at[steps])
    weights.start()
    for i in range(steps):
        rows = pl.ds(i * CHUNK, CHUNK)
        copy = pltpu.make_async_copy(x_ref.at[rows], held.at[rows], sems.at[i])
        copy.start()
        copies.append(copy)
    weights.wait()
    parts = both_parts(held_w[...])
    out_ref[:, total:] = held_w[...]
    for i in range(steps):
        rows = pl.ds(i * CHUNK, CHUNK)
        copies[i].wait()
        x = held[rows, :]
        high = x.astype(BF16)
        low = (x - high.astype(F32)).astype(BF16)
        high_ref[rows, :] = high
        low_ref[rows, :] = low
        out_ref[:, rows] = product_of(parts, high, low, NT)


def chip_kernel(recv_ref, weights_ref, out_ref):
    rows = out_ref.shape[2]
    weights_ref[...] = jnp.concatenate([recv_ref[0, :, rows:], recv_ref[1, :, rows:]], axis=1)
    spread(out_ref, sum_first(recv_ref, 0, rows))


def grad_kernel(recv_ref, labels_ref, high1, low1, logits_ref, probs_ref, parts_ref, half_ref):
    logits = sum_first(recv_ref)
    logits_ref[...] = logits
    expo = jnp.exp(logits)
    probs = expo / jnp.sum(expo, axis=0, keepdims=True)
    probs_ref[...] = probs
    onehot = (labels_ref[...] == lax.broadcasted_iota(jnp.int32, logits.shape, 0)).astype(F32)
    parts = both_parts(probs - onehot)
    parts_ref[...] = parts
    half_ref[...] = product_of(parts, high1[...], low1[...], NN)


def moved_kernel(parts_ref, half_ref, moved_ref, out_ref, high0_ref, low0_ref):
    x = moved_ref[...]
    high = x.astype(BF16)
    high0_ref[...] = high
    low0_ref[...] = (x - high.astype(F32)).astype(BF16)
    first = product_of(parts_ref[...], high0_ref[...], low0_ref[...], NN)
    spread_blocks(out_ref, jnp.concatenate([first, half_ref[...]], axis=1))


def resid_kernel(count, recv_ref, w_ref, high0, low0, high1, low1, resid_ref, out_ref):
    resid = -(joined(recv_ref) / count + RIDGE * w_ref[...])
    resid_ref[...] = resid
    spread(out_ref, chip_rows(resid, ((high0, low0), (high1, low1))))


def product_kernel(count, recv_ref, resid_ref, high0, low0, high1, low1, product_ref, out_ref):
    resid = resid_ref[...]
    product = joined(recv_ref) / count + RIDGE * resid
    product_ref[...] = product
    tile = tile_of(*(total_of(a * b) for a, b in ((resid, resid), (resid, product), (product, product))))
    image = chip_rows(product, ((high0, low0), (high1, low1)))
    rows = image.shape[1]
    for i in range(out_ref.shape[0]):
        out_ref[i, :, :rows] = image
        out_ref[i, :, rows:] = tile


def image_kernel(recv_ref, probs_ref, high0, low0, high1, low1, image_ref, out_ref):
    image = sum_first(recv_ref)
    image_ref[...] = image
    chip_columns(out_ref, curved(probs_ref[...], image), ((high0, low0), (high1, low1)))


def scalars(tail):
    rr0, along, square = tail[:1, :1], tail[:1, 1:2], tail[:1, 2:3]
    alpha = rr0 / along
    rr1 = jnp.maximum(rr0 - 2.0 * alpha * along + alpha * alpha * square, 0.0)
    return rr0, alpha, rr1, rr1 / rr0


def second_kernel(recv_ref, probs_ref, image_ref, direction_ref, tail_ref, out_ref):
    rows = image_ref.shape[1]
    tail = sum_first(recv_ref, rows, rows + LANES)
    tail_ref[...] = tail
    rr0, alpha, rr1, beta = scalars(tail)
    image = image_ref[...]
    direction = image - alpha * sum_first(recv_ref, 0, rows) + beta * image
    direction_ref[...] = direction
    curvature = total_of(direction * curved(probs_ref[...], direction))
    out_ref[...] = jnp.broadcast_to(curvature, out_ref.shape)


def last_kernel(
    count, curvature_ref, tail_ref, w_ref, resid_ref, product_ref, logits_ref,
    image_ref, direction_ref, out_ref,
):
    rows = logits_ref.shape[1]
    rr0, alpha, rr1, beta = scalars(tail_ref[...])
    curvature = sum_first(curvature_ref)[:, :1]
    bent = curvature / count + RIDGE * (rr1 + beta * beta * rr0)
    alpha1 = jnp.where(rr1 > 0.0, rr1 / bent, 0.0)
    resid = resid_ref[...]
    direction = resid - alpha * product_ref[...] + beta * resid
    out_ref[:, rows:] = w_ref[...] + (alpha * resid + alpha1 * direction)
    out_ref[:, :rows] = logits_ref[...] + (alpha * image_ref[...] + alpha1 * direction_ref[...])


def share_kernel(recv_ref, weights_ref, scores_ref):
    rows, width = scores_ref.shape[1], weights_ref.shape[1]
    scores_ref[...] = recv_ref[1, :, :rows]
    start = pl.multiple_of(rows + width * lax.axis_index("core"), LANES)
    weights_ref[...] = recv_ref[1, :, pl.ds(start, width)]


def call(kernel, shapes, *args, in_specs=None, scratch=(), limit=4):
    shapes = [jax.ShapeDtypeStruct(s, F32) if isinstance(s, tuple) else s for s in shapes]
    vmem = pl.BlockSpec(memory_space=pltpu.VMEM)
    return pl.pallas_call(
        kernel,
        out_shape=shapes,
        in_specs=in_specs or [vmem] * len(args),
        out_specs=[vmem] * len(shapes),
        scratch_shapes=list(scratch),
        compiler_params=pltpu.CompilerParams(vmem_limit_bytes=limit * 1024 * 1024),
    )(*args)


def groups(kind):
    nx, nz, ny, nc = (lax.axis_size(axis) for axis in GRID)
    place = np.arange(nx * nz * ny * nc).reshape(nx, nz, ny, nc)
    near, work = place[..., 0], place[..., 1]
    xyz = near.transpose(1, 0, 2)
    if kind == "x":
        pair = work.transpose(2, 1, 0).reshape(-1, nx), near.reshape(-1, ny)
    elif kind == "y":
        pair = work.reshape(-1, ny), near.transpose(1, 2, 0).reshape(-1, nx)
    elif kind == "z":
        pair = work.transpose(0, 2, 1).reshape(-1, nz), xyz.reshape(-1, nx * ny)
    else:
        pair = work.transpose(2, 0, 1).reshape(ny, -1), xyz.reshape(ny, -1)
    return np.concatenate(pair).tolist()


def exchange(blocks, kind):
    return lax.all_to_all(blocks, GRID, 0, 0, axis_index_groups=groups(kind), tiled=True)


def relay(recv, axis):
    (blocks,) = call(relay_kernel, [(lax.axis_size(axis), *recv.shape[1:])], recv)
    return exchange(blocks, axis)


def over_cells(blocks):
    return relay(relay(exchange(blocks, "x"), "z"), "x")


def on_device(features, labels, weights):
    rows, width = features.shape
    classes = weights.shape[0]
    count = rows * lax.axis_size(CELLS) * 1.0
    split = pltpu.VMEM((rows, width), BF16)
    planes, lines = lax.axis_size("x"), lax.axis_size("y")
    cells, coeffs, tile = (classes, rows), (classes, 2 * width), (classes, LANES)
    blocks = (planes, classes, 2 * width // planes)
    padded = (lines, classes, rows + LANES)

    high1, low1, partial, held = call(
        first_kernel,
        [
            split,
            split,
            pltpu.VMEM((classes, rows + width), F32),
            pltpu.VMEM((rows, width), F32),
        ],
        weights,
        features,
        in_specs=[pl.BlockSpec(memory_space=pltpu.HBM)] * 2,
        limit=49,
        scratch=[
            pltpu.VMEM((classes, width), F32),
            pltpu.SemaphoreType.DMA((rows // CHUNK + 1,)),
        ],
    )
    gathered, held = lax.optimization_barrier((lax.all_gather(partial, "core"), held))
    moved = lax.ppermute(held, "core", [(0, 1)])
    weights, partial = call(chip_kernel, [coeffs, (lines, *cells)], gathered)
    logits, probs, terms, half = call(
        grad_kernel,
        [cells, cells, pltpu.VMEM((2 * classes, rows), BF16), (classes, width)],
        exchange(partial, "y"), labels.reshape(1, rows), high1, low1,
    )
    partial, high0, low0 = call(moved_kernel, [blocks, split, split], terms, half, moved)
    parts = (high0, low0, high1, low1)
    resid, partial = call(
        functools.partial(resid_kernel, count), [coeffs, (lines, *cells)], over_cells(partial), weights, *parts
    )
    image, partial = call(
        image_kernel, [cells, blocks], exchange(partial, "y"), probs, *parts
    )
    product, partial = call(
        functools.partial(product_kernel, count), [coeffs, padded], over_cells(partial), resid, *parts
    )
    direction, tail, curvature = call(
        second_kernel,
        [cells, tile, (lax.axis_size(CELLS), 1, LANES)],
        exchange(partial, "y"), probs, image,
    )
    (result,) = call(
        functools.partial(last_kernel, count),
        [(classes, rows + 2 * width)],
        exchange(curvature, "cells"), tail, weights, resid, product, logits, image, direction,
    )
    return tuple(
        call(share_kernel, [(classes, width), cells], lax.all_gather(result, "core"))
    )


def solution(mesh):
    grid = Mesh(mesh.devices.reshape(4, 16, 4, 2), GRID)
    return jax.shard_map(
        on_device,
        mesh=grid,
        in_specs=(P(CELLS, FEAT), P(CELLS), P(None, FEAT)),
        out_specs=(P(None, FEAT), P(None, CELLS)),
        check_vma=False,
    )
```

```python
import functools

import jax
import jax.numpy as jnp
import numpy as np
from jax import lax
from jax.experimental import pallas as pl
from jax.experimental.pallas import tpu as pltpu
from jax.sharding import Mesh, PartitionSpec as P

RIDGE = 0.01
CELLS = ("x", "z")
GRID = ("x", "z", "y", "core")
FEAT = ("y", "core")
LANES = 128
CHUNK = 512
F32 = jnp.float32
BF16 = jnp.bfloat16
NN = (((1,), (0,)), ((), ()))
NT = (((1,), (1,)), ((), ()))


def both_parts(value):
    high = value.astype(BF16).astype(F32)
    return jnp.concatenate([high, value - high], axis=0).astype(BF16)


def product_of(parts, high, low, dims):
    k = parts.shape[0] // 2
    one = lax.dot_general(parts, high, dims, preferred_element_type=F32)
    two = lax.dot_general(parts, low, dims, preferred_element_type=F32)
    total = one + two
    return total[:k] + total[k:]


def sum_first(ref, lo=None, hi=None):
    total = ref[0] if lo is None else ref[0, :, lo:hi]
    for i in range(1, ref.shape[0]):
        total = total + (ref[i] if lo is None else ref[i, :, lo:hi])
    return total


def joined(ref):
    return jnp.concatenate([ref[i] for i in range(ref.shape[0])], axis=1)


def curved(probs, image):
    weighted = probs * image
    return weighted - probs * jnp.sum(weighted, axis=0, keepdims=True)


def total_of(value):
    return jnp.sum(jnp.sum(value, axis=1, keepdims=True), axis=0, keepdims=True)


def tile_of(first, second):
    column = lax.broadcasted_iota(jnp.int32, (8, LANES), 1)
    return jnp.where(column == 0, first, jnp.where(column == 1, second, 0.0))


def spread(ref, value):
    for i in range(ref.shape[0]):
        ref[i] = value


def spread_blocks(ref, value):
    step = value.shape[1] // ref.shape[0]
    for i in range(ref.shape[0]):
        ref[i] = value[:, i * step : (i + 1) * step]


def relay_kernel(recv_ref, out_ref):
    spread(out_ref, sum_first(recv_ref))


def chip_rows(value, parts_of):
    (high0, low0), (high1, low1) = parts_of
    half = value.shape[1] // 2
    left = product_of(both_parts(value[:, :half]), high0[...], low0[...], NT)
    return left + product_of(both_parts(value[:, half:]), high1[...], low1[...], NT)


def chip_columns(ref, value, parts_of):
    parts = both_parts(value)
    halves = [product_of(parts, high[...], low[...], NN) for high, low in parts_of]
    spread_blocks(ref, jnp.concatenate(halves, axis=1))


def first_kernel(w_ref, x_ref, high_ref, low_ref, out_ref, held, held_w, sems):
    total = held.shape[0]
    steps = total // CHUNK
    copies = []
    weights = pltpu.make_async_copy(w_ref, held_w, sems.at[steps])
    weights.start()
    for i in range(steps):
        rows = pl.ds(i * CHUNK, CHUNK)
        copy = pltpu.make_async_copy(x_ref.at[rows], held.at[rows], sems.at[i])
        copy.start()
        copies.append(copy)
    weights.wait()
    parts = both_parts(held_w[...])
    out_ref[:, total:] = held_w[...]
    for i in range(steps):
        rows = pl.ds(i * CHUNK, CHUNK)
        copies[i].wait()
        x = held[rows, :]
        high = x.astype(BF16)
        low = (x - high.astype(F32)).astype(BF16)
        high_ref[rows, :] = high
        low_ref[rows, :] = low
        out_ref[:, rows] = product_of(parts, high, low, NT)


def chip_kernel(recv_ref, weights_ref, out_ref):
    rows = out_ref.shape[2]
    weights_ref[...] = jnp.concatenate([recv_ref[0, :, rows:], recv_ref[1, :, rows:]], axis=1)
    spread(out_ref, sum_first(recv_ref, 0, rows))


def grad_kernel(recv_ref, labels_ref, high1, low1, logits_ref, probs_ref, parts_ref, half_ref):
    logits = sum_first(recv_ref)
    logits_ref[...] = logits
    expo = jnp.exp(logits)
    probs = expo / jnp.sum(expo, axis=0, keepdims=True)
    probs_ref[...] = probs
    onehot = (labels_ref[...] == lax.broadcasted_iota(jnp.int32, logits.shape, 0)).astype(F32)
    parts = both_parts(probs - onehot)
    parts_ref[...] = parts
    half_ref[...] = product_of(parts, high1[...], low1[...], NN)


def moved_kernel(parts_ref, half_ref, moved_ref, out_ref, high0_ref, low0_ref):
    x = moved_ref[...]
    high = x.astype(BF16)
    high0_ref[...] = high
    low0_ref[...] = (x - high.astype(F32)).astype(BF16)
    first = product_of(parts_ref[...], high0_ref[...], low0_ref[...], NN)
    spread_blocks(out_ref, jnp.concatenate([first, half_ref[...]], axis=1))


def send_rows(out_ref, value, tile, parts_of):
    rows = out_ref.shape[2] - LANES
    image = chip_rows(value, parts_of)
    for i in range(out_ref.shape[0]):
        out_ref[i, :, :rows] = image
        out_ref[i, :, rows:] = tile


def resid_kernel(count, recv_ref, w_ref, high0, low0, high1, low1, resid_ref, out_ref):
    resid = -(joined(recv_ref) / count + RIDGE * w_ref[...])
    resid_ref[...] = resid
    tile = tile_of(total_of(resid * resid), 0.0)
    send_rows(out_ref, resid, tile, ((high0, low0), (high1, low1)))


def product_kernel(count, recv_ref, resid_ref, high0, low0, high1, low1, product_ref, out_ref):
    resid = resid_ref[...]
    product = joined(recv_ref) / count + RIDGE * resid
    product_ref[...] = product
    tile = tile_of(total_of(resid * product), total_of(product * product))
    send_rows(out_ref, product, tile, ((high0, low0), (high1, low1)))


def image_kernel(recv_ref, probs_ref, high0, low0, high1, low1, image_ref, tail_ref, out_ref):
    rows = image_ref.shape[1]
    image = sum_first(recv_ref, 0, rows)
    image_ref[...] = image
    tail_ref[...] = sum_first(recv_ref, rows, rows + LANES)
    chip_columns(out_ref, curved(probs_ref[...], image), ((high0, low0), (high1, low1)))


def scalars(rr0, tail):
    along, square = tail[:1, :1], tail[:1, 1:2]
    alpha = rr0 / along
    rr1 = jnp.maximum(rr0 - 2.0 * alpha * along + alpha * alpha * square, 0.0)
    return alpha, rr1, rr1 / rr0


def second_kernel(recv_ref, tail_ref, probs_ref, image_ref, direction_ref, tail2_ref, out_ref):
    rows = image_ref.shape[1]
    tail = sum_first(recv_ref, rows, rows + LANES)
    tail2_ref[...] = tail
    alpha, rr1, beta = scalars(tail_ref[:1, :1], tail)
    image = image_ref[...]
    direction = image - alpha * sum_first(recv_ref, 0, rows) + beta * image
    direction_ref[...] = direction
    curvature = total_of(direction * curved(probs_ref[...], direction))
    out_ref[...] = jnp.broadcast_to(curvature, out_ref.shape)


def last_kernel(
    count, curvature_ref, tail_ref, tail2_ref, w_ref, resid_ref, product_ref, logits_ref,
    image_ref, direction_ref, out_ref,
):
    rows = logits_ref.shape[1]
    rr0 = tail_ref[:1, :1]
    alpha, rr1, beta = scalars(rr0, tail2_ref[...])
    curvature = sum_first(curvature_ref)[:, :1]
    bent = curvature / count + RIDGE * (rr1 + beta * beta * rr0)
    alpha1 = jnp.where(rr1 > 0.0, rr1 / bent, 0.0)
    resid = resid_ref[...]
    direction = resid - alpha * product_ref[...] + beta * resid
    out_ref[:, rows:] = w_ref[...] + (alpha * resid + alpha1 * direction)
    out_ref[:, :rows] = logits_ref[...] + (alpha * image_ref[...] + alpha1 * direction_ref[...])


def share_kernel(recv_ref, weights_ref, scores_ref):
    rows, width = scores_ref.shape[1], weights_ref.shape[1]
    scores_ref[...] = recv_ref[1, :, :rows]
    start = pl.multiple_of(rows + width * lax.axis_index("core"), LANES)
    weights_ref[...] = recv_ref[1, :, pl.ds(start, width)]


def call(kernel, shapes, *args, in_specs=None, scratch=(), limit=4):
    shapes = [jax.ShapeDtypeStruct(s, F32) if isinstance(s, tuple) else s for s in shapes]
    vmem = pl.BlockSpec(memory_space=pltpu.VMEM)
    return pl.pallas_call(
        kernel,
        out_shape=shapes,
        in_specs=in_specs or [vmem] * len(args),
        out_specs=[vmem] * len(shapes),
        scratch_shapes=list(scratch),
        compiler_params=pltpu.CompilerParams(vmem_limit_bytes=limit * 1024 * 1024),
    )(*args)


def groups(kind):
    nx, nz, ny, nc = (lax.axis_size(axis) for axis in GRID)
    place = np.arange(nx * nz * ny * nc).reshape(nx, nz, ny, nc)
    near, work = place[..., 0], place[..., 1]
    xyz = near.transpose(1, 0, 2)
    if kind == "x":
        pair = work.transpose(2, 1, 0).reshape(-1, nx), near.reshape(-1, ny)
    elif kind == "y":
        pair = work.reshape(-1, ny), near.transpose(1, 2, 0).reshape(-1, nx)
    elif kind == "z":
        order = np.arange(nz) * 7 % nz
        pair = work[:, order].transpose(0, 2, 1).reshape(-1, nz), xyz.reshape(-1, nx * ny)
    else:
        pair = work.transpose(2, 0, 1).reshape(ny, -1), xyz.reshape(ny, -1)
    return np.concatenate(pair).tolist()


def exchange(blocks, kind):
    return lax.all_to_all(blocks, GRID, 0, 0, axis_index_groups=groups(kind), tiled=True)


def relay(recv, axis):
    (blocks,) = call(relay_kernel, [(lax.axis_size(axis), *recv.shape[1:])], recv)
    return exchange(blocks, axis)


def over_cells(blocks):
    return relay(relay(exchange(blocks, "x"), "z"), "x")


def on_device(features, labels, weights):
    rows, width = features.shape
    classes = weights.shape[0]
    count = rows * lax.axis_size(CELLS) * 1.0
    split = pltpu.VMEM((rows, width), BF16)
    planes, lines = lax.axis_size("x"), lax.axis_size("y")
    cells, coeffs, tile = (classes, rows), (classes, 2 * width), (classes, LANES)
    blocks = (planes, classes, 2 * width // planes)
    padded = (lines, classes, rows + LANES)

    high1, low1, partial, held = call(
        first_kernel,
        [
            split,
            split,
            pltpu.VMEM((classes, rows + width), F32),
            pltpu.VMEM((rows, width), F32),
        ],
        weights,
        features,
        in_specs=[pl.BlockSpec(memory_space=pltpu.HBM)] * 2,
        limit=49,
        scratch=[
            pltpu.VMEM((classes, width), F32),
            pltpu.SemaphoreType.DMA((rows // CHUNK + 1,)),
        ],
    )
    gathered, held = lax.optimization_barrier((lax.all_gather(partial, "core"), held))
    moved = lax.ppermute(held, "core", [(0, 1)])
    weights, partial = call(chip_kernel, [coeffs, (lines, *cells)], gathered)
    logits, probs, terms, half = call(
        grad_kernel,
        [cells, cells, pltpu.VMEM((2 * classes, rows), BF16), (classes, width)],
        exchange(partial, "y"), labels.reshape(1, rows), high1, low1,
    )
    partial, high0, low0 = call(moved_kernel, [blocks, split, split], terms, half, moved)
    parts = (high0, low0, high1, low1)
    resid, partial = call(
        functools.partial(resid_kernel, count), [coeffs, padded], over_cells(partial), weights, *parts
    )
    image, tail, partial = call(
        image_kernel, [cells, tile, blocks], exchange(partial, "y"), probs, *parts
    )
    product, partial = call(
        functools.partial(product_kernel, count), [coeffs, padded], over_cells(partial), resid, *parts
    )
    direction, tail2, curvature = call(
        second_kernel,
        [cells, tile, (lax.axis_size(CELLS), 1, LANES)],
        exchange(partial, "y"), tail, probs, image,
    )
    (result,) = call(
        functools.partial(last_kernel, count),
        [(classes, rows + 2 * width)],
        exchange(curvature, "cells"), tail, tail2, weights, resid, product, logits, image, direction,
    )
    return tuple(
        call(share_kernel, [(classes, width), cells], lax.all_gather(result, "core"))
    )


def solution(mesh):
    grid = Mesh(mesh.devices.reshape(4, 16, 4, 2), GRID)
    return jax.shard_map(
        on_device,
        mesh=grid,
        in_specs=(P(CELLS, FEAT), P(CELLS), P(None, FEAT)),
        out_specs=(P(None, FEAT), P(None, CELLS)),
        check_vma=False,
    )
```

```python
import functools

import jax
import jax.numpy as jnp
import numpy as np
from jax import lax
from jax.experimental import pallas as pl
from jax.experimental.pallas import tpu as pltpu
from jax.sharding import Mesh, PartitionSpec as P

RIDGE = 0.01
CELLS = ("x", "z")
GRID = ("x", "z", "y", "core")
FEAT = ("y", "core")
LANES = 128
CHUNK = 512
F32 = jnp.float32
BF16 = jnp.bfloat16
NN = (((1,), (0,)), ((), ()))
NT = (((1,), (1,)), ((), ()))


def both_parts(value):
    high = value.astype(BF16).astype(F32)
    return jnp.concatenate([high, value - high], axis=0).astype(BF16)


def product_of(parts, high, low, dims):
    k = parts.shape[0] // 2
    one = lax.dot_general(parts, high, dims, preferred_element_type=F32)
    two = lax.dot_general(parts, low, dims, preferred_element_type=F32)
    total = one + two
    return total[:k] + total[k:]


def sum_first(ref, lo=None, hi=None):
    total = ref[0] if lo is None else ref[0, :, lo:hi]
    for i in range(1, ref.shape[0]):
        total = total + (ref[i] if lo is None else ref[i, :, lo:hi])
    return total


def joined(ref):
    return jnp.concatenate([ref[i] for i in range(ref.shape[0])], axis=1)


def curved(probs, image):
    weighted = probs * image
    return weighted - probs * jnp.sum(weighted, axis=0, keepdims=True)


def total_of(value):
    return jnp.sum(jnp.sum(value, axis=1, keepdims=True), axis=0, keepdims=True)


def tile_of(first, second):
    column = lax.broadcasted_iota(jnp.int32, (8, LANES), 1)
    return jnp.where(column == 0, first, jnp.where(column == 1, second, 0.0))


def spread(ref, value):
    for i in range(ref.shape[0]):
        ref[i] = value


def spread_blocks(ref, value):
    step = value.shape[1] // ref.shape[0]
    for i in range(ref.shape[0]):
        ref[i] = value[:, i * step : (i + 1) * step]


def relay_kernel(recv_ref, out_ref):
    spread(out_ref, sum_first(recv_ref))


def chip_rows(value, parts_of):
    (high0, low0), (high1, low1) = parts_of
    half = value.shape[1] // 2
    left = product_of(both_parts(value[:, :half]), high0[...], low0[...], NT)
    return left + product_of(both_parts(value[:, half:]), high1[...], low1[...], NT)


def chip_columns(ref, value, parts_of):
    parts = both_parts(value)
    halves = [product_of(parts, high[...], low[...], NN) for high, low in parts_of]
    spread_blocks(ref, jnp.concatenate(halves, axis=1))


def first_kernel(w_ref, x_ref, high_ref, low_ref, out_ref, held, held_w, sems):
    total = held.shape[0]
    steps = total // CHUNK
    copies = []
    weights = pltpu.make_async_copy(w_ref, held_w, sems.at[steps])
    weights.start()
    for i in range(steps):
        rows = pl.ds(i * CHUNK, CHUNK)
        copy = pltpu.make_async_copy(x_ref.at[rows], held.at[rows], sems.at[i])
        copy.start()
        copies.append(copy)
    weights.wait()
    parts = both_parts(held_w[...])
    out_ref[:, total:] = held_w[...]
    for i in range(steps):
        rows = pl.ds(i * CHUNK, CHUNK)
        copies[i].wait()
        x = held[rows, :]
        high = x.astype(BF16)
        low = (x - high.astype(F32)).astype(BF16)
        high_ref[rows, :] = high
        low_ref[rows, :] = low
        out_ref[:, rows] = product_of(parts, high, low, NT)


def chip_kernel(recv_ref, weights_ref, out_ref):
    rows = out_ref.shape[2]
    weights_ref[...] = jnp.concatenate([recv_ref[0, :, rows:], recv_ref[1, :, rows:]], axis=1)
    spread(out_ref, sum_first(recv_ref, 0, rows))


def grad_kernel(recv_ref, labels_ref, high1, low1, logits_ref, probs_ref, parts_ref, half_ref):
    logits = sum_first(recv_ref)
    logits_ref[...] = logits
    expo = jnp.exp(logits)
    probs = expo / jnp.sum(expo, axis=0, keepdims=True)
    probs_ref[...] = probs
    onehot = (labels_ref[...] == lax.broadcasted_iota(jnp.int32, logits.shape, 0)).astype(F32)
    parts = both_parts(probs - onehot)
    parts_ref[...] = parts
    half_ref[...] = product_of(parts, high1[...], low1[...], NN)


def moved_kernel(parts_ref, half_ref, moved_ref, out_ref, high0_ref, low0_ref):
    x = moved_ref[...]
    high = x.astype(BF16)
    high0_ref[...] = high
    low0_ref[...] = (x - high.astype(F32)).astype(BF16)
    first = product_of(parts_ref[...], high0_ref[...], low0_ref[...], NN)
    spread_blocks(out_ref, jnp.concatenate([first, half_ref[...]], axis=1))


def send_rows(out_ref, value, tile, parts_of):
    rows = out_ref.shape[2] - LANES
    image = chip_rows(value, parts_of)
    for i in range(out_ref.shape[0]):
        out_ref[i, :, :rows] = image
        out_ref[i, :, rows:] = tile


def resid_kernel(count, recv_ref, w_ref, high0, low0, high1, low1, resid_ref, out_ref):
    resid = -(joined(recv_ref) / count + RIDGE * w_ref[...])
    resid_ref[...] = resid
    tile = tile_of(total_of(resid * resid), 0.0)
    send_rows(out_ref, resid, tile, ((high0, low0), (high1, low1)))


def product_kernel(count, recv_ref, resid_ref, high0, low0, high1, low1, product_ref, out_ref):
    resid = resid_ref[...]
    product = joined(recv_ref) / count + RIDGE * resid
    product_ref[...] = product
    tile = tile_of(total_of(resid * product), total_of(product * product))
    send_rows(out_ref, product, tile, ((high0, low0), (high1, low1)))


def image_kernel(recv_ref, probs_ref, high0, low0, high1, low1, image_ref, tail_ref, out_ref):
    rows = image_ref.shape[1]
    image = sum_first(recv_ref, 0, rows)
    image_ref[...] = image
    tail_ref[...] = sum_first(recv_ref, rows, rows + LANES)
    chip_columns(out_ref, curved(probs_ref[...], image), ((high0, low0), (high1, low1)))


def scalars(rr0, tail):
    along, square = tail[:1, :1], tail[:1, 1:2]
    alpha = rr0 / along
    rr1 = jnp.maximum(rr0 - 2.0 * alpha * along + alpha * alpha * square, 0.0)
    return alpha, rr1, rr1 / rr0


def second_kernel(recv_ref, tail_ref, probs_ref, image_ref, direction_ref, tail2_ref, out_ref):
    rows = image_ref.shape[1]
    tail = sum_first(recv_ref, rows, rows + LANES)
    tail2_ref[...] = tail
    alpha, rr1, beta = scalars(tail_ref[:1, :1], tail)
    image = image_ref[...]
    direction = image - alpha * sum_first(recv_ref, 0, rows) + beta * image
    direction_ref[...] = direction
    curvature = total_of(direction * curved(probs_ref[...], direction))
    out_ref[...] = jnp.broadcast_to(curvature, out_ref.shape)


def last_kernel(
    count, curvature_ref, tail_ref, tail2_ref, w_ref, resid_ref, product_ref, logits_ref,
    image_ref, direction_ref, out_ref,
):
    rows = logits_ref.shape[1]
    rr0 = tail_ref[:1, :1]
    alpha, rr1, beta = scalars(rr0, tail2_ref[...])
    curvature = sum_first(curvature_ref)[:, :1]
    bent = curvature / count + RIDGE * (rr1 + beta * beta * rr0)
    alpha1 = jnp.where(rr1 > 0.0, rr1 / bent, 0.0)
    resid = resid_ref[...]
    direction = resid - alpha * product_ref[...] + beta * resid
    out_ref[:, rows:] = w_ref[...] + (alpha * resid + alpha1 * direction)
    out_ref[:, :rows] = logits_ref[...] + (alpha * image_ref[...] + alpha1 * direction_ref[...])


def share_kernel(recv_ref, weights_ref, scores_ref, sems):
    rows, width = scores_ref.shape[1], weights_ref.shape[1]
    start = pl.multiple_of(rows + width * lax.axis_index("core"), LANES)
    scores = pltpu.make_async_copy(recv_ref.at[1, :, pl.ds(0, rows)], scores_ref, sems.at[0])
    weights = pltpu.make_async_copy(recv_ref.at[1, :, pl.ds(start, width)], weights_ref, sems.at[1])
    scores.start()
    weights.start()
    scores.wait()
    weights.wait()


def call(kernel, shapes, *args, in_specs=None, space=pltpu.VMEM, scratch=(), limit=4):
    shapes = [jax.ShapeDtypeStruct(s, F32) if isinstance(s, tuple) else s for s in shapes]
    vmem = pl.BlockSpec(memory_space=pltpu.VMEM)
    return pl.pallas_call(
        kernel,
        out_shape=shapes,
        in_specs=in_specs or [vmem] * len(args),
        out_specs=[pl.BlockSpec(memory_space=space)] * len(shapes),
        scratch_shapes=list(scratch),
        compiler_params=pltpu.CompilerParams(vmem_limit_bytes=limit * 1024 * 1024),
    )(*args)


def groups(kind):
    nx, nz, ny, nc = (lax.axis_size(axis) for axis in GRID)
    place = np.arange(nx * nz * ny * nc).reshape(nx, nz, ny, nc)
    near, work = place[..., 0], place[..., 1]
    xyz = near.transpose(1, 0, 2)
    if kind == "x":
        pair = work.transpose(2, 1, 0).reshape(-1, nx), near.reshape(-1, ny)
    elif kind == "y":
        pair = work.reshape(-1, ny), near.transpose(1, 2, 0).reshape(-1, nx)
    elif kind == "z":
        pair = work.transpose(0, 2, 1).reshape(-1, nz), xyz.reshape(-1, nx * ny)
    else:
        pair = work.transpose(2, 0, 1).reshape(ny, -1), xyz.reshape(ny, -1)
    return np.concatenate(pair).tolist()


def exchange(blocks, kind):
    return lax.all_to_all(blocks, GRID, 0, 0, axis_index_groups=groups(kind), tiled=True)


def relay(recv, axis):
    (blocks,) = call(relay_kernel, [(lax.axis_size(axis), *recv.shape[1:])], recv)
    return exchange(blocks, axis)


def over_cells(blocks):
    return relay(relay(exchange(blocks, "x"), "z"), "x")


def on_device(features, labels, weights):
    rows, width = features.shape
    classes = weights.shape[0]
    count = rows * lax.axis_size(CELLS) * 1.0
    split = pltpu.VMEM((rows, width), BF16)
    planes, lines = lax.axis_size("x"), lax.axis_size("y")
    cells, coeffs, tile = (classes, rows), (classes, 2 * width), (classes, LANES)
    blocks = (planes, classes, 2 * width // planes)
    padded = (lines, classes, rows + LANES)

    high1, low1, partial, held = call(
        first_kernel,
        [
            split,
            split,
            pltpu.VMEM((classes, rows + width), F32),
            pltpu.VMEM((rows, width), F32),
        ],
        weights,
        features,
        in_specs=[pl.BlockSpec(memory_space=pltpu.HBM)] * 2,
        limit=49,
        scratch=[
            pltpu.VMEM((classes, width), F32),
            pltpu.SemaphoreType.DMA((rows // CHUNK + 1,)),
        ],
    )
    gathered, held = lax.optimization_barrier((lax.all_gather(partial, "core"), held))
    moved = lax.ppermute(held, "core", [(0, 1)])
    weights, partial = call(chip_kernel, [coeffs, (lines, *cells)], gathered)
    logits, probs, terms, half = call(
        grad_kernel,
        [cells, cells, pltpu.VMEM((2 * classes, rows), BF16), (classes, width)],
        exchange(partial, "y"), labels.reshape(1, rows), high1, low1,
    )
    partial, high0, low0 = call(moved_kernel, [blocks, split, split], terms, half, moved)
    parts = (high0, low0, high1, low1)
    resid, partial = call(
        functools.partial(resid_kernel, count), [coeffs, padded], over_cells(partial), weights, *parts
    )
    image, tail, partial = call(
        image_kernel, [cells, tile, blocks], exchange(partial, "y"), probs, *parts
    )
    product, partial = call(
        functools.partial(product_kernel, count), [coeffs, padded], over_cells(partial), resid, *parts
    )
    direction, tail2, curvature = call(
        second_kernel,
        [cells, tile, (lax.axis_size(CELLS), 1, LANES)],
        exchange(partial, "y"), tail, probs, image,
    )
    (result,) = call(
        functools.partial(last_kernel, count),
        [(classes, rows + 2 * width)],
        exchange(curvature, "cells"), tail, tail2, weights, resid, product, logits, image, direction,
    )
    return tuple(
        call(
            share_kernel,
            [(classes, width), cells],
            lax.all_gather(result, "core"),
            space=pltpu.HBM,
            scratch=[pltpu.SemaphoreType.DMA((2,))],
        )
    )


def solution(mesh):
    grid = Mesh(mesh.devices.reshape(4, 16, 4, 2), GRID)
    return jax.shard_map(
        on_device,
        mesh=grid,
        in_specs=(P(CELLS, FEAT), P(CELLS), P(None, FEAT)),
        out_specs=(P(None, FEAT), P(None, CELLS)),
        check_vma=False,
    )
```

```python
import functools

import jax
import jax.numpy as jnp
import numpy as np
from jax import lax
from jax.experimental import pallas as pl
from jax.experimental.pallas import tpu as pltpu
from jax.sharding import Mesh, PartitionSpec as P

RIDGE = 0.01
CELLS = ("x", "z")
GRID = ("x", "z", "y", "core")
FEAT = ("y", "core")
LANES = 128
CHUNK = 1024
F32 = jnp.float32
BF16 = jnp.bfloat16
NN = (((1,), (0,)), ((), ()))
NT = (((1,), (1,)), ((), ()))


def both_parts(value):
    high = value.astype(BF16).astype(F32)
    return jnp.concatenate([high, value - high], axis=0).astype(BF16)


def product_of(parts, high, low, dims):
    k = parts.shape[0] // 2
    one = lax.dot_general(parts, high, dims, preferred_element_type=F32)
    two = lax.dot_general(parts, low, dims, preferred_element_type=F32)
    total = one + two
    return total[:k] + total[k:]


def sum_first(ref, lo=None, hi=None):
    total = ref[0] if lo is None else ref[0, :, lo:hi]
    for i in range(1, ref.shape[0]):
        total = total + (ref[i] if lo is None else ref[i, :, lo:hi])
    return total


def joined(ref):
    return jnp.concatenate([ref[i] for i in range(ref.shape[0])], axis=1)


def curved(probs, image):
    weighted = probs * image
    return weighted - probs * jnp.sum(weighted, axis=0, keepdims=True)


def total_of(value):
    return jnp.sum(jnp.sum(value, axis=1, keepdims=True), axis=0, keepdims=True)


def tile_of(first, second):
    column = lax.broadcasted_iota(jnp.int32, (8, LANES), 1)
    return jnp.where(column == 0, first, jnp.where(column == 1, second, 0.0))


def spread(ref, value):
    for i in range(ref.shape[0]):
        ref[i] = value


def spread_blocks(ref, value):
    step = value.shape[1] // ref.shape[0]
    for i in range(ref.shape[0]):
        ref[i] = value[:, i * step : (i + 1) * step]


def relay_kernel(recv_ref, out_ref):
    spread(out_ref, sum_first(recv_ref))


def chip_rows(value, parts_of):
    (high0, low0), (high1, low1) = parts_of
    half = value.shape[1] // 2
    left = product_of(both_parts(value[:, :half]), high0[...], low0[...], NT)
    return left + product_of(both_parts(value[:, half:]), high1[...], low1[...], NT)


def chip_columns(ref, value, parts_of):
    parts = both_parts(value)
    halves = [product_of(parts, high[...], low[...], NN) for high, low in parts_of]
    spread_blocks(ref, jnp.concatenate(halves, axis=1))


def first_kernel(w_ref, x_ref, high_ref, low_ref, out_ref, held, held_w, sems):
    total = held.shape[0]
    steps = total // CHUNK
    copies = []
    weights = pltpu.make_async_copy(w_ref, held_w, sems.at[steps])
    weights.start()
    for i in range(steps):
        rows = pl.ds(i * CHUNK, CHUNK)
        copy = pltpu.make_async_copy(x_ref.at[rows], held.at[rows], sems.at[i])
        copy.start()
        copies.append(copy)
    weights.wait()
    parts = both_parts(held_w[...])
    out_ref[:, total:] = held_w[...]
    for i in range(steps):
        rows = pl.ds(i * CHUNK, CHUNK)
        copies[i].wait()
        x = held[rows, :]
        high = x.astype(BF16)
        low = (x - high.astype(F32)).astype(BF16)
        high_ref[rows, :] = high
        low_ref[rows, :] = low
        out_ref[:, rows] = product_of(parts, high, low, NT)


def chip_kernel(recv_ref, weights_ref, out_ref):
    rows = out_ref.shape[2]
    weights_ref[...] = jnp.concatenate([recv_ref[0, :, rows:], recv_ref[1, :, rows:]], axis=1)
    spread(out_ref, sum_first(recv_ref, 0, rows))


def grad_kernel(recv_ref, labels_ref, high1, low1, logits_ref, probs_ref, parts_ref, half_ref):
    logits = sum_first(recv_ref)
    logits_ref[...] = logits
    expo = jnp.exp(logits)
    probs = expo / jnp.sum(expo, axis=0, keepdims=True)
    probs_ref[...] = probs
    onehot = (labels_ref[...] == lax.broadcasted_iota(jnp.int32, logits.shape, 0)).astype(F32)
    parts = both_parts(probs - onehot)
    parts_ref[...] = parts
    half_ref[...] = product_of(parts, high1[...], low1[...], NN)


def moved_kernel(parts_ref, half_ref, moved_ref, out_ref, high0_ref, low0_ref):
    x = moved_ref[...]
    high = x.astype(BF16)
    high0_ref[...] = high
    low0_ref[...] = (x - high.astype(F32)).astype(BF16)
    first = product_of(parts_ref[...], high0_ref[...], low0_ref[...], NN)
    spread_blocks(out_ref, jnp.concatenate([first, half_ref[...]], axis=1))


def send_rows(out_ref, value, tile, parts_of):
    rows = out_ref.shape[2] - LANES
    image = chip_rows(value, parts_of)
    for i in range(out_ref.shape[0]):
        out_ref[i, :, :rows] = image
        out_ref[i, :, rows:] = tile


def resid_kernel(count, recv_ref, w_ref, high0, low0, high1, low1, resid_ref, out_ref):
    resid = -(joined(recv_ref) / count + RIDGE * w_ref[...])
    resid_ref[...] = resid
    tile = tile_of(total_of(resid * resid), 0.0)
    send_rows(out_ref, resid, tile, ((high0, low0), (high1, low1)))


def product_kernel(count, recv_ref, resid_ref, high0, low0, high1, low1, product_ref, out_ref):
    resid = resid_ref[...]
    product = joined(recv_ref) / count + RIDGE * resid
    product_ref[...] = product
    tile = tile_of(total_of(resid * product), total_of(product * product))
    send_rows(out_ref, product, tile, ((high0, low0), (high1, low1)))


def image_kernel(recv_ref, probs_ref, high0, low0, high1, low1, image_ref, tail_ref, out_ref):
    rows = image_ref.shape[1]
    image = sum_first(recv_ref, 0, rows)
    image_ref[...] = image
    tail_ref[...] = sum_first(recv_ref, rows, rows + LANES)
    chip_columns(out_ref, curved(probs_ref[...], image), ((high0, low0), (high1, low1)))


def scalars(rr0, tail):
    along, square = tail[:1, :1], tail[:1, 1:2]
    alpha = rr0 / along
    rr1 = jnp.maximum(rr0 - 2.0 * alpha * along + alpha * alpha * square, 0.0)
    return alpha, rr1, rr1 / rr0


def second_kernel(recv_ref, tail_ref, probs_ref, image_ref, direction_ref, tail2_ref, out_ref):
    rows = image_ref.shape[1]
    tail = sum_first(recv_ref, rows, rows + LANES)
    tail2_ref[...] = tail
    alpha, rr1, beta = scalars(tail_ref[:1, :1], tail)
    image = image_ref[...]
    direction = image - alpha * sum_first(recv_ref, 0, rows) + beta * image
    direction_ref[...] = direction
    curvature = total_of(direction * curved(probs_ref[...], direction))
    out_ref[...] = jnp.broadcast_to(curvature, out_ref.shape)


def last_kernel(
    count, curvature_ref, tail_ref, tail2_ref, w_ref, resid_ref, product_ref, logits_ref,
    image_ref, direction_ref, out_ref,
):
    rows = logits_ref.shape[1]
    rr0 = tail_ref[:1, :1]
    alpha, rr1, beta = scalars(rr0, tail2_ref[...])
    curvature = sum_first(curvature_ref)[:, :1]
    bent = curvature / count + RIDGE * (rr1 + beta * beta * rr0)
    alpha1 = jnp.where(rr1 > 0.0, rr1 / bent, 0.0)
    resid = resid_ref[...]
    direction = resid - alpha * product_ref[...] + beta * resid
    out_ref[:, rows:] = w_ref[...] + (alpha * resid + alpha1 * direction)
    out_ref[:, :rows] = logits_ref[...] + (alpha * image_ref[...] + alpha1 * direction_ref[...])


def share_kernel(recv_ref, weights_ref, scores_ref):
    rows, width = scores_ref.shape[1], weights_ref.shape[1]
    scores_ref[...] = recv_ref[1, :, :rows]
    start = pl.multiple_of(rows + width * lax.axis_index("core"), LANES)
    weights_ref[...] = recv_ref[1, :, pl.ds(start, width)]


def call(kernel, shapes, *args, in_specs=None, scratch=(), limit=4):
    shapes = [jax.ShapeDtypeStruct(s, F32) if isinstance(s, tuple) else s for s in shapes]
    vmem = pl.BlockSpec(memory_space=pltpu.VMEM)
    return pl.pallas_call(
        kernel,
        out_shape=shapes,
        in_specs=in_specs or [vmem] * len(args),
        out_specs=[vmem] * len(shapes),
        scratch_shapes=list(scratch),
        compiler_params=pltpu.CompilerParams(vmem_limit_bytes=limit * 1024 * 1024),
    )(*args)


def groups(kind):
    nx, nz, ny, nc = (lax.axis_size(axis) for axis in GRID)
    place = np.arange(nx * nz * ny * nc).reshape(nx, nz, ny, nc)
    near, work = place[..., 0], place[..., 1]
    xyz = near.transpose(1, 0, 2)
    if kind == "x":
        pair = work.transpose(2, 1, 0).reshape(-1, nx), near.reshape(-1, ny)
    elif kind == "y":
        pair = work.reshape(-1, ny), near.transpose(1, 2, 0).reshape(-1, nx)
    elif kind == "z":
        pair = work.transpose(0, 2, 1).reshape(-1, nz), xyz.reshape(-1, nx * ny)
    else:
        pair = work.transpose(2, 0, 1).reshape(ny, -1), xyz.reshape(ny, -1)
    return np.concatenate(pair).tolist()


def exchange(blocks, kind):
    return lax.all_to_all(blocks, GRID, 0, 0, axis_index_groups=groups(kind), tiled=True)


def relay(recv, axis):
    (blocks,) = call(relay_kernel, [(lax.axis_size(axis), *recv.shape[1:])], recv)
    return exchange(blocks, axis)


def over_cells(blocks):
    return relay(relay(exchange(blocks, "x"), "z"), "x")


def on_device(features, labels, weights):
    rows, width = features.shape
    classes = weights.shape[0]
    count = rows * lax.axis_size(CELLS) * 1.0
    split = pltpu.VMEM((rows, width), BF16)
    planes, lines = lax.axis_size("x"), lax.axis_size("y")
    cells, coeffs, tile = (classes, rows), (classes, 2 * width), (classes, LANES)
    blocks = (planes, classes, 2 * width // planes)
    padded = (lines, classes, rows + LANES)

    high1, low1, partial, held = call(
        first_kernel,
        [
            split,
            split,
            pltpu.VMEM((classes, rows + width), F32),
            pltpu.VMEM((rows, width), F32),
        ],
        weights,
        features,
        in_specs=[pl.BlockSpec(memory_space=pltpu.HBM)] * 2,
        limit=49,
        scratch=[
            pltpu.VMEM((classes, width), F32),
            pltpu.SemaphoreType.DMA((rows // CHUNK + 1,)),
        ],
    )
    gathered, held = lax.optimization_barrier((lax.all_gather(partial, "core"), held))
    moved = lax.ppermute(held, "core", [(0, 1)])
    weights, partial = call(chip_kernel, [coeffs, (lines, *cells)], gathered)
    logits, probs, terms, half = call(
        grad_kernel,
        [cells, cells, pltpu.VMEM((2 * classes, rows), BF16), (classes, width)],
        exchange(partial, "y"), labels.reshape(1, rows), high1, low1,
    )
    partial, high0, low0 = call(moved_kernel, [blocks, split, split], terms, half, moved)
    parts = (high0, low0, high1, low1)
    resid, partial = call(
        functools.partial(resid_kernel, count), [coeffs, padded], over_cells(partial), weights, *parts
    )
    image, tail, partial = call(
        image_kernel, [cells, tile, blocks], exchange(partial, "y"), probs, *parts
    )
    product, partial = call(
        functools.partial(product_kernel, count), [coeffs, padded], over_cells(partial), resid, *parts
    )
    direction, tail2, curvature = call(
        second_kernel,
        [cells, tile, (lax.axis_size(CELLS), 1, LANES)],
        exchange(partial, "y"), tail, probs, image,
    )
    (result,) = call(
        functools.partial(last_kernel, count),
        [(classes, rows + 2 * width)],
        exchange(curvature, "cells"), tail, tail2, weights, resid, product, logits, image, direction,
    )
    return tuple(
        call(share_kernel, [(classes, width), cells], lax.all_gather(result, "core"))
    )


def solution(mesh):
    grid = Mesh(mesh.devices.reshape(4, 16, 4, 2), GRID)
    return jax.shard_map(
        on_device,
        mesh=grid,
        in_specs=(P(CELLS, FEAT), P(CELLS), P(None, FEAT)),
        out_specs=(P(None, FEAT), P(None, CELLS)),
        check_vma=False,
    )
```
